128 devices in a mesh: farcp: 2 (over x_lo), nearcp: 8 (over z_hi, x_hi, core), model: 8 (over z_lo, y).
Axes of the slice: x: 4 (x_hi: 2, x_lo: 2; x = x_hi * 2 + x_lo), y: 4, z: 4 (z_hi: 2, z_lo: 2; z = z_hi * 2 + z_lo), core: 2. Of those that a mesh axis runs over, the one named last changes fastest.
Arguments:
- raw_keys: bfloat16 [16, 16384, 8, 128], P(None, ('farcp', 'nearcp'), 'model'), may hold values from -6 to 6
- raw_values: bfloat16 [16, 16384, 8, 128], P(None, ('farcp', 'nearcp'), 'model'), may hold values from -6 to 6
- turn_angle: float32 [16384, 64], replicated, may hold values from -3.140625 to 3.140625
- key_gain: float32 [128], replicated, may hold values from 0.25 to 1.75
Outputs:
- stored_keys: bfloat16 [16, 16384, 8, 128], P(('farcp', 'nearcp'), None, 'model')
- stored_values: bfloat16 [16, 16384, 8, 128], P(('farcp', 'nearcp'), None, 'model')
- key_scale: float32 [16, 8, 128], P(('farcp', 'nearcp'), 'model')
The draws below stay inside these ranges and needn't reach their ends.
All inputs are finite; a program needn't handle non-finite values. Where the reference program divides by a largest or mean magnitude, that divisor is 1e-20 or more.
Results may differ from the reference program's by a relative error of at most 0.001.
Values may be sent and summed in bfloat16 or wider, within the bound.
A program may use at most 192 MiB of HBM per device.

```python
import jax
import jax.numpy as jnp
from jax import lax

BATCH = 16
LENGTH = 16384
KV_HEADS = 8
HEAD_SIZE = 128
HALF_HEAD = 64


def steps_of(rng, extent, cuts, low, largest):
    loudness = 1.0
    for dim, shards_of in cuts:
        draws = jax.random.uniform(jax.random.fold_in(jax.random.fold_in(rng, 6), dim), (shards_of,), jnp.float32, low / len(cuts), largest / len(cuts))
        loudness = loudness * jnp.repeat(jnp.exp(draws), extent[dim] // shards_of).reshape((-1,) + (1,) * (len(extent) - 1 - dim))
    return loudness


def gaussian(stream_key, extent, scale, reach, pieces=(), dtype=jnp.bfloat16):
    array = scale * jax.random.normal(stream_key, extent, jnp.float32)
    if pieces:
        array = array * steps_of(stream_key, extent, pieces, -0.22, 0.18)
    return jnp.clip(array, -reach, reach).astype(dtype)


def setup_inputs(seed: int = 0) -> dict:
    keys = jax.random.split(jax.random.key(seed), 5)
    return {
        "raw_keys": gaussian(keys[0], (BATCH, LENGTH, KV_HEADS, HEAD_SIZE), 1.0, 6.0, ((1, 16), (2, 8))),
        "raw_values": gaussian(keys[1], (BATCH, LENGTH, KV_HEADS, HEAD_SIZE), 1.0, 6.0, ((1, 16), (2, 8))),
        "turn_angle": jnp.clip(jax.random.uniform(keys[2], (LENGTH, HALF_HEAD), jnp.float32, -3.140625, 3.140625), -3.140625, 3.140625),
        "key_gain": jnp.clip(1.0 + 0.15 * jax.random.normal(keys[3], (HEAD_SIZE,), jnp.float32), 0.25, 1.75),
    }


def apply_rotary(vectors, angle):
    half = vectors.shape[-1] // 2
    cosine, sine = (jnp.cos(angle)[None, :, None, :], jnp.sin(angle)[None, :, None, :])
    first, second = (vectors[..., :half], vectors[..., half:])
    return jnp.concatenate([first * cosine - second * sine, second * cosine + first * sine], axis=-1)

def scale_rows(vectors, row_gain):
    return vectors * lax.rsqrt(lax.optimization_barrier(jnp.mean(vectors * vectors, axis=-1, keepdims=True)) + 1e-06) * row_gain

def prepare_keys(plain_keys, angle, key_gain):
    wide_keys = plain_keys.astype(jnp.float32)
    wide_keys = scale_rows(wide_keys, key_gain)
    return apply_rotary(wide_keys, angle)

def reference(raw_keys, raw_values, turn_angle, key_gain):
    turned_keys = prepare_keys(raw_keys, turn_angle, key_gain)
    key_scale = lax.optimization_barrier(jnp.max(jnp.abs(turned_keys), axis=1))
    narrow_keys = (turned_keys / key_scale[:, None]).astype(jnp.bfloat16)
    stored_keys = narrow_keys
    stored_values = raw_values
    return (stored_keys, stored_values, key_scale)
```

```python
import jax
import jax.numpy as jnp
from jax import lax
from jax.experimental import pallas as pl
from jax.experimental.pallas import tpu as pltpu
from jax.sharding import PartitionSpec as P

MESH = pl.DeviceIdType.MESH
SEQS, ROWS, LANES, HALF = 16, 1024, 128, 64
TOTAL = SEQS * ROWS
CHUNK = 128
FIRST_ROWS = 512


def interleave(a, b):
    merged = []
    for i in range(max(len(a), len(b))):
        merged += a[i : i + 1] + b[i : i + 1]
    return merged


ALONG_Z = [(0, 1, c) for c in (0, 1)]
ALONG_X = [(dx, 0, c) for c in (0, 1) for dx in (1, 3, 2)]
DIAGONAL = [(dx, 1, c) for c in (0, 1) for dx in (1, 3, 2)]
ORDER = interleave(ALONG_Z + DIAGONAL, ALONG_X) + [(0, 0, 1)]
PEERS = len(ORDER)


def exchange(
    keys, values, angle, gain,
    kland, vland, scale,
    raw, turned, narrow, angles, gains_row, cosines, sines, maxes,
    local_sem, v_send, v_recv, k_send, k_recv, m_send, m_recv,
):
    far, near, model = lax.axis_index("farcp"), lax.axis_index("nearcp"), lax.axis_index("model")
    core, x, z = near % 2, ((near // 2) % 2) * 2 + far, near // 4
    me = far * 8 + near

    def place(dx, dz, dc):
        px, pz, pc = (x + dx) % 4, (z + dz) % 2, (core + dc) % 2
        return px % 2, pz * 4 + (px // 2) * 2 + pc

    peers = [place(*step) for step in ORDER]
    ids = [(f, n, model) for f, n in peers]
    index = [f * 8 + n for f, n in peers]

    load_keys = pltpu.make_async_copy(keys, raw, local_sem.at[0])
    load_angles = pltpu.make_async_copy(
        angle.at[:, pl.ds(pl.multiple_of(me * ROWS, ROWS), ROWS)], angles, local_sem.at[1]
    )
    keep = pltpu.make_async_copy(
        values.at[me], vland.at[pl.ds(pl.multiple_of(me * ROWS, ROWS), ROWS)], local_sem.at[2]
    )
    load_keys.start()
    load_angles.start()
    load_gain = pltpu.make_async_copy(gain, gains_row, local_sem.at[3])
    load_gain.start()

    barrier = pltpu.get_barrier_semaphore()
    for device in ids:
        pl.semaphore_signal(barrier, inc=1, device_id=device, device_id_type=MESH)
    pl.semaphore_wait(barrier, PEERS)

    def send_values(part, first, rows):
        copies = [
            pltpu.make_async_remote_copy(
                src_ref=values.at[index[i], pl.ds(first, rows)],
                dst_ref=vland.at[pl.ds(pl.multiple_of(me * ROWS + first, CHUNK), rows)],
                send_sem=v_send.at[part, i],
                recv_sem=v_recv.at[part, i],
                device_id=ids[i],
                device_id_type=MESH,
            )
            for i in range(PEERS)
        ]
        for copy in copies:
            copy.start()
        return copies

    copies = send_values(0, 0, FIRST_ROWS)
    keep.start()

    load_angles.wait()
    for c in range(ROWS // CHUNK):
        a = angles[:, c * CHUNK : (c + 1) * CHUNK]
        cosine, sine = jnp.cos(a), jnp.sin(a)
        rows = pl.ds(c * CHUNK, CHUNK)
        cosines[rows, :] = jnp.concatenate([cosine, cosine], axis=0).T
        sines[rows, :] = jnp.concatenate([-sine, sine], axis=0).T

    load_keys.wait()
    load_gain.wait()
    gains = gains_row[...]

    def turn_sequence(s, _):
        def turn_rows(c, largest):
            rows = pl.ds(pl.multiple_of(c * CHUNK, CHUNK), CHUNK)
            wide = raw[s, rows, :].astype(jnp.float32)
            mean = jnp.mean(wide * wide, axis=-1, keepdims=True)
            wide = wide * lax.rsqrt(mean + 1e-06) * gains
            out = wide * cosines[rows, :] + pltpu.roll(wide, HALF, 1) * sines[rows, :]
            turned[s, rows, :] = out
            return jnp.maximum(largest, jnp.max(jnp.abs(out).reshape(CHUNK // 8, 8, LANES), axis=0))

        largest = lax.fori_loop(0, ROWS // CHUNK, turn_rows, jnp.zeros((8, LANES), jnp.float32))
        maxes[0, pl.ds(s, 1), :] = jnp.max(largest, axis=0, keepdims=True)
        return 0

    lax.fori_loop(0, SEQS, turn_sequence, 0)

    shared = [
        pltpu.make_async_remote_copy(
            src_ref=maxes.at[0],
            dst_ref=maxes.at[1 + i],
            send_sem=m_send.at[i],
            recv_sem=m_recv.at[i],
            device_id=ids[i],
            device_id_type=MESH,
        )
        for i in range(PEERS)
    ]
    for copy in shared:
        copy.start()
    copies += send_values(1, FIRST_ROWS, ROWS - FIRST_ROWS)
    for copy in shared:
        copy.wait()

    largest = maxes[0]
    for i in range(PEERS):
        largest = jnp.maximum(largest, maxes[1 + i])
    maxes[0] = largest
    scale[...] = maxes[0, pl.ds(me, 1), :]

    def scale_sequence(s, _):
        inverse = 1.0 / maxes[0, pl.ds(s, 1), :]

        def scale_rows(c, _):
            rows = pl.ds(pl.multiple_of(c * CHUNK, CHUNK), CHUNK)
            narrow[s, rows, :] = (turned[s, rows, :] * inverse).astype(jnp.bfloat16)
            return 0

        lax.fori_loop(0, ROWS // CHUNK, scale_rows, 0)
        return 0

    lax.fori_loop(0, SEQS, scale_sequence, 0)

    sent = [
        pltpu.make_async_remote_copy(
            src_ref=narrow.at[index[i]],
            dst_ref=kland.at[pl.ds(pl.multiple_of(me * ROWS, ROWS), ROWS)],
            send_sem=k_send.at[i],
            recv_sem=k_recv.at[i],
            device_id=ids[i],
            device_id_type=MESH,
        )
        for i in range(PEERS)
    ]
    for copy in sent:
        copy.start()

    def keep_rows(c, _):
        rows = pl.ds(pl.multiple_of(me * ROWS + c * CHUNK, CHUNK), CHUNK)
        kland[rows, :] = narrow[me, pl.ds(pl.multiple_of(c * CHUNK, CHUNK), CHUNK), :]
        return 0

    lax.fori_loop(0, ROWS // CHUNK, keep_rows, 0)
    keep.wait()
    for copy in copies + sent:
        copy.wait()


PIECES = 8


def store(kland, vland, scale, kout, vout, scale_out, sems):
    rows = TOTAL // PIECES
    copies = []
    for i, (source, target) in enumerate(((kland, kout), (vland, vout))):
        for j in range(PIECES):
            part = pl.ds(j * rows, rows)
            copies.append(pltpu.make_async_copy(source.at[part], target.at[part], sems.at[i, j]))
    copies.append(pltpu.make_async_copy(scale, scale_out, sems.at[2, 0]))
    for copy in copies:
        copy.start()
    for copy in copies:
        copy.wait()


def local(raw_keys, raw_values, turn_angle, key_gain):
    shape = (SEQS, ROWS, LANES)
    hbm = pl.BlockSpec(memory_space=pltpu.HBM)
    vmem = pl.BlockSpec(memory_space=pltpu.VMEM)
    kland, vland, scale = pl.pallas_call(
        exchange,
        name="exchange",
        out_shape=(
            pltpu.VMEM((TOTAL, LANES), jnp.bfloat16),
            pltpu.VMEM((TOTAL, LANES), jnp.bfloat16),
            pltpu.VMEM((1, LANES), jnp.float32),
        ),
        in_specs=[hbm, hbm, hbm, hbm],
        out_specs=(vmem, vmem, vmem),
        scratch_shapes=[
            pltpu.VMEM(shape, jnp.bfloat16),
            pltpu.VMEM(shape, jnp.float32),
            pltpu.VMEM(shape, jnp.bfloat16),
            pltpu.VMEM((HALF, ROWS), jnp.float32),
            pltpu.VMEM((1, LANES), jnp.float32),
            pltpu.VMEM((ROWS, LANES), jnp.float32),
            pltpu.VMEM((ROWS, LANES), jnp.float32),
            pltpu.VMEM((1 + PEERS, SEQS, LANES), jnp.float32),
            pltpu.SemaphoreType.DMA((4,)),
            pltpu.SemaphoreType.DMA((2, PEERS)),
            pltpu.SemaphoreType.DMA((2, PEERS)),
            pltpu.SemaphoreType.DMA((PEERS,)),
            pltpu.SemaphoreType.DMA((PEERS,)),
            pltpu.SemaphoreType.DMA((PEERS,)),
            pltpu.SemaphoreType.DMA((PEERS,)),
        ],
        compiler_params=pltpu.CompilerParams(
            collective_id=0, has_side_effects=True, vmem_limit_bytes=40 * 2**20
        ),
    )(
        *(
            pltpu.with_memory_space_constraint(array, pltpu.HBM)
            for array in (
                raw_keys.reshape(shape),
                raw_values.reshape(shape),
                turn_angle.T,
                key_gain.reshape(1, LANES),
            )
        )
    )
    kout, vout, scale = pl.pallas_call(
        store,
        name="store",
        out_shape=(
            jax.ShapeDtypeStruct((TOTAL, LANES), jnp.bfloat16),
            jax.ShapeDtypeStruct((TOTAL, LANES), jnp.bfloat16),
            jax.ShapeDtypeStruct((1, LANES), jnp.float32),
        ),
        in_specs=[vmem, vmem, vmem],
        out_specs=(hbm, hbm, hbm),
        scratch_shapes=[pltpu.SemaphoreType.DMA((3, PIECES))],
        compiler_params=pltpu.CompilerParams(vmem_limit_bytes=2**20),
    )(kland, vland, scale)
    whole = (1, TOTAL, 1, LANES)
    return kout.reshape(whole), vout.reshape(whole), scale.reshape(1, 1, LANES)


def solution(mesh):
    in_specs = (
        P(None, ("farcp", "nearcp"), "model", None),
        P(None, ("farcp", "nearcp"), "model", None),
        P(),
        P(),
    )
    out_specs = (
        P(("farcp", "nearcp"), None, "model", None),
        P(("farcp", "nearcp"), None, "model", None),
        P(("farcp", "nearcp"), "model", None),
    )
    return jax.shard_map(local, mesh=mesh, in_specs=in_specs, out_specs=out_specs, check_vma=False)
```

```python
import jax
import jax.numpy as jnp
from jax import lax
from jax.experimental import pallas as pl
from jax.experimental.pallas import tpu as pltpu
from jax.sharding import PartitionSpec as P

MESH = pl.DeviceIdType.MESH
SEQS, ROWS, LANES, HALF = 16, 1024, 128, 64
TOTAL = SEQS * ROWS
CHUNK = 128
FIRST_ROWS = 768
Z_FIRST = 3
V_ONE, V_TWO = 2, 4


STEPS = [(dx, c) for c in (0, 1) for dx in (1, 3, 2)]
RELAYED = len(STEPS)
PLANE = RELAYED + 1
COPIES = 64


def exchange(
    keys, values, angle, gain,
    kland, vland, scale,
    raw, turned, narrow, krelay, vrelay, angles, gains_row, cosines, sines, maxes,
    local_sem, send_sem, recv_sem,
):
    far, near, model = lax.axis_index("farcp"), lax.axis_index("nearcp"), lax.axis_index("model")
    core, x, z = near % 2, ((near // 2) % 2) * 2 + far, near // 4
    used = [0]

    def place(dx, dz, dc):
        px, pz, pc = (x + dx) % 4, (z + dz) % 2, (core + dc) % 2
        return px % 2, pz * 4 + (px // 2) * 2 + pc

    def device(dx, dz, dc):
        return (*place(dx, dz, dc), model)

    def index(dx, dz, dc):
        f, n = place(dx, dz, dc)
        return f * 8 + n

    def block(owner, first=0, rows=ROWS):
        return pl.ds(pl.multiple_of(owner * ROWS + first, CHUNK), rows)

    me, across = far * 8 + near, index(0, 1, 0)

    def send(source, target, *step):
        i = used[0]
        used[0] += 1
        copy = pltpu.make_async_remote_copy(
            src_ref=source,
            dst_ref=target,
            send_sem=send_sem.at[i],
            recv_sem=recv_sem.at[i],
            device_id=device(*step),
            device_id_type=MESH,
        )
        copy.start()
        return copy

    load_keys = pltpu.make_async_copy(keys, raw, local_sem.at[0])
    load_angles = pltpu.make_async_copy(angle.at[:, block(me)], angles, local_sem.at[1])
    load_gain = pltpu.make_async_copy(gain, gains_row, local_sem.at[2])
    keep = pltpu.make_async_copy(values.at[me], vland.at[block(me)], local_sem.at[3])

    barrier = pltpu.get_barrier_semaphore()
    greeted = [(0, 1, 0), (0, 1, 1), (0, 0, 1)] + [(dx, 0, dc) for dx, dc in STEPS]
    for step in greeted:
        pl.semaphore_signal(barrier, inc=1, device_id=device(*step), device_id_type=MESH)
    load_angles.start()
    load_gain.start()
    load_keys.start()
    pl.semaphore_wait(barrier, len(greeted))

    def relay_out(source, relay, i):
        dx, dc = STEPS[i]
        return send(source.at[index(dx, 1, dc)], relay.at[i], 0, 1, 0)

    def forward(relay, land, i):
        dx, dc = STEPS[i]
        return send(relay.at[i], land.at[block(across)], dx, 0, dc)

    def along_x(source, land, i, first, rows):
        dx, dc = STEPS[i]
        part = pl.ds(first, rows)
        return send(source.at[index(dx, 0, dc), part], land.at[block(me, first, rows)], dx, 0, dc)

    def along_z(source, land, dc):
        return send(source.at[index(0, 1, dc)], land.at[block(me)], 0, 1, dc)

    def to_sibling(source, land):
        return send(source.at[index(0, 0, 1)], land.at[block(me)], 0, 0, 1)

    vz, copies = [], []
    for i in range(RELAYED):
        if i < Z_FIRST:
            vz.append(relay_out(values, vrelay, i))
        copies.append(along_x(values, vland, i, 0, FIRST_ROWS))
    copies.append(to_sibling(values, vland))
    keep.start()

    load_angles.wait()
    for c in range(ROWS // CHUNK):
        a = angles[:, c * CHUNK : (c + 1) * CHUNK]
        cosine, sine = jnp.cos(a), jnp.sin(a)
        rows = pl.ds(c * CHUNK, CHUNK)
        cosines[rows, :] = jnp.concatenate([cosine, cosine], axis=0).T
        sines[rows, :] = jnp.concatenate([-sine, sine], axis=0).T

    load_gain.wait()
    load_keys.wait()
    gains = gains_row[...]

    def turn_sequence(s, _):
        largest = jnp.zeros((8, LANES), jnp.float32)
        for c in range(ROWS // CHUNK):
            rows = pl.ds(c * CHUNK, CHUNK)
            wide = raw[s, rows, :].astype(jnp.float32)
            mean = jnp.mean(wide * wide, axis=-1, keepdims=True)
            wide = wide * lax.rsqrt(mean + 1e-06) * gains
            out = wide * cosines[rows, :] + pltpu.roll(wide, HALF, 1) * sines[rows, :]
            turned[s, rows, :] = out
            largest = jnp.maximum(
                largest, jnp.max(jnp.abs(out).reshape(CHUNK // 8, 8, LANES), axis=0)
            )
        maxes[0, pl.ds(s, 1), :] = jnp.max(largest, axis=0, keepdims=True)
        return 0

    lax.fori_loop(0, SEQS, turn_sequence, 0)

    first = send(maxes.at[0], maxes.at[1], 0, 1, 0)
    for i in range(Z_FIRST, RELAYED):
        vz.append(relay_out(values, vrelay, i))
    for dc in (0, 1):
        copies.append(along_z(values, vland, dc))
    if FIRST_ROWS < ROWS:
        for i in range(RELAYED):
            copies.append(along_x(values, vland, i, FIRST_ROWS, ROWS - FIRST_ROWS))
    for i in range(V_ONE):
        vz[i].wait_recv()
        copies.append(forward(vrelay, vland, i))
    first.wait()
    maxes[2] = jnp.maximum(maxes[0], maxes[1])
    second = [
        send(maxes.at[2], maxes.at[3 + i], dx, 0, dc) for i, (dx, dc) in enumerate(STEPS + [(0, 1)])
    ]
    for i in range(V_ONE, V_TWO):
        vz[i].wait_recv()
        copies.append(forward(vrelay, vland, i))
    for copy in second:
        copy.wait()
    largest = maxes[2]
    for i in range(PLANE):
        largest = jnp.maximum(largest, maxes[3 + i])
    maxes[0] = largest
    scale[...] = maxes[0, pl.ds(me, 1), :]

    def scale_sequence(s, _):
        inverse = 1.0 / maxes[0, pl.ds(s, 1), :]
        for c in range(ROWS // CHUNK):
            rows = pl.ds(c * CHUNK, CHUNK)
            narrow[s, rows, :] = (turned[s, rows, :] * inverse).astype(jnp.bfloat16)
        return 0

    lax.fori_loop(0, SEQS, scale_sequence, 0)

    kz = [relay_out(narrow, krelay, i) for i in range(RELAYED)]
    for dc in (0, 1):
        copies.append(along_z(narrow, kland, dc))
    for i in range(V_TWO, RELAYED):
        vz[i].wait_recv()
        copies.append(forward(vrelay, vland, i))
    for i in range(RELAYED):
        copies.append(along_x(narrow, kland, i, 0, ROWS))
    copies.append(to_sibling(narrow, kland))

    def keep_rows(c, _):
        kland[block(me, c * CHUNK, CHUNK), :] = narrow[
            me, pl.ds(pl.multiple_of(c * CHUNK, CHUNK), CHUNK), :
        ]
        return 0

    lax.fori_loop(0, ROWS // CHUNK, keep_rows, 0)
    for i in range(RELAYED):
        kz[i].wait_recv()
        copies.append(forward(krelay, kland, i))
    keep.wait()
    for copy in vz + kz:
        copy.wait_send()
    for copy in copies:
        copy.wait()


PIECES = 8


def store(kland, vland, scale, kout, vout, scale_out, sems):
    rows = TOTAL // PIECES
    copies = []
    for i, (source, target) in enumerate(((kland, kout), (vland, vout))):
        for j in range(PIECES):
            part = pl.ds(j * rows, rows)
            copies.append(pltpu.make_async_copy(source.at[part], target.at[part], sems.at[i, j]))
    copies.append(pltpu.make_async_copy(scale, scale_out, sems.at[2, 0]))
    for copy in copies:
        copy.start()
    for copy in copies:
        copy.wait()


def local(raw_keys, raw_values, turn_angle, key_gain):
    shape = (SEQS, ROWS, LANES)
    hbm = pl.BlockSpec(memory_space=pltpu.HBM)
    vmem = pl.BlockSpec(memory_space=pltpu.VMEM)
    kland, vland, scale = pl.pallas_call(
        exchange,
        name="exchange",
        out_shape=(
            pltpu.VMEM((TOTAL, LANES), jnp.bfloat16),
            pltpu.VMEM((TOTAL, LANES), jnp.bfloat16),
            pltpu.VMEM((1, LANES), jnp.float32),
        ),
        in_specs=[hbm, hbm, hbm, hbm],
        out_specs=(vmem, vmem, vmem),
        scratch_shapes=[
            pltpu.VMEM(shape, jnp.bfloat16),
            pltpu.VMEM(shape, jnp.float32),
            pltpu.VMEM(shape, jnp.bfloat16),
            pltpu.VMEM((RELAYED, ROWS, LANES), jnp.bfloat16),
            pltpu.VMEM((RELAYED, ROWS, LANES), jnp.bfloat16),
            pltpu.VMEM((HALF, ROWS), jnp.float32),
            pltpu.VMEM((1, LANES), jnp.float32),
            pltpu.VMEM((ROWS, LANES), jnp.float32),
            pltpu.VMEM((ROWS, LANES), jnp.float32),
            pltpu.VMEM((3 + PLANE, SEQS, LANES), jnp.float32),
            pltpu.SemaphoreType.DMA((4,)),
            pltpu.SemaphoreType.DMA((COPIES,)),
            pltpu.SemaphoreType.DMA((COPIES,)),
        ],
        compiler_params=pltpu.CompilerParams(
            collective_id=0, has_side_effects=True, vmem_limit_bytes=40 * 2**20
        ),
    )(
        *(
            pltpu.with_memory_space_constraint(array, pltpu.HBM)
            for array in (
                raw_keys.reshape(shape),
                raw_values.reshape(shape),
                turn_angle.T,
                key_gain.reshape(1, LANES),
            )
        )
    )
    kout, vout, scale = pl.pallas_call(
        store,
        name="store",
        out_shape=(
            jax.ShapeDtypeStruct((TOTAL, LANES), jnp.bfloat16),
            jax.ShapeDtypeStruct((TOTAL, LANES), jnp.bfloat16),
            jax.ShapeDtypeStruct((1, LANES), jnp.float32),
        ),
        in_specs=[vmem, vmem, vmem],
        out_specs=(hbm, hbm, hbm),
        scratch_shapes=[pltpu.SemaphoreType.DMA((3, PIECES))],
        compiler_params=pltpu.CompilerParams(vmem_limit_bytes=2**20),
    )(kland, vland, scale)
    whole = (1, TOTAL, 1, LANES)
    return kout.reshape(whole), vout.reshape(whole), scale.reshape(1, 1, LANES)


def solution(mesh):
    in_specs = (
        P(None, ("farcp", "nearcp"), "model", None),
        P(None, ("farcp", "nearcp"), "model", None),
        P(),
        P(),
    )
    out_specs = (
        P(("farcp", "nearcp"), None, "model", None),
        P(("farcp", "nearcp"), None, "model", None),
        P(("farcp", "nearcp"), "model", None),
    )
    return jax.shard_map(local, mesh=mesh, in_specs=in_specs, out_specs=out_specs, check_vma=False)
```

```python
import jax
import jax.numpy as jnp
from jax import lax
from jax.experimental import pallas as pl
from jax.experimental.pallas import tpu as pltpu
from jax.sharding import PartitionSpec as P

MESH = pl.DeviceIdType.MESH
SEQS, ROWS, LANES, HALF = 16, 1024, 128, 64
TOTAL = SEQS * ROWS
CHUNK = 128
FIRST_ROWS = 768
Z_FIRST = 3
V_ONE, V_TWO = 2, 4


STEPS = [(dx, c) for c in (0, 1) for dx in (1, 3, 2)]
RELAYED = len(STEPS)
PLANE = RELAYED + 1
COPIES = 64


def exchange(
    keys, values, angle, gain,
    kland, vland, scale,
    raw, turned, narrow, krelay, vrelay, angles, gains_row, cosines, sines, maxes,
    local_sem, ready_sem, send_sem, recv_sem,
):
    far, near, model = lax.axis_index("farcp"), lax.axis_index("nearcp"), lax.axis_index("model")
    core, x, z = near % 2, ((near // 2) % 2) * 2 + far, near // 4
    used = [0]

    def place(dx, dz, dc):
        px, pz, pc = (x + dx) % 4, (z + dz) % 2, (core + dc) % 2
        return px % 2, pz * 4 + (px // 2) * 2 + pc

    def device(dx, dz, dc):
        return (*place(dx, dz, dc), model)

    def index(dx, dz, dc):
        f, n = place(dx, dz, dc)
        return f * 8 + n

    def block(owner, first=0, rows=ROWS):
        return pl.ds(pl.multiple_of(owner * ROWS + first, CHUNK), rows)

    me, across = far * 8 + near, index(0, 1, 0)

    def plan(source, target, *step):
        i = used[0]
        used[0] += 1
        return pltpu.make_async_remote_copy(
            src_ref=source,
            dst_ref=target,
            send_sem=send_sem.at[i],
            recv_sem=recv_sem.at[i],
            device_id=device(*step),
            device_id_type=MESH,
        )

    def start(copies):
        for copy in copies:
            copy.start()

    def send(*way):
        copy = plan(*way)
        copy.start()
        return copy

    load_keys = pltpu.make_async_copy(keys, raw, local_sem.at[0])
    load_angles = pltpu.make_async_copy(angle.at[:, block(me)], angles, local_sem.at[1])
    load_gain = pltpu.make_async_copy(gain, gains_row, local_sem.at[2])
    keep = pltpu.make_async_copy(values.at[me], vland.at[block(me)], local_sem.at[3])

    barrier = pltpu.get_barrier_semaphore()
    greeted = [device(0, 1, core), device(0, 0, 1)] + [device(dx, 0, 1 - core) for dx in (1, 3, 2)]
    for target in greeted:
        pl.semaphore_signal(barrier, inc=1, device_id=target, device_id_type=MESH)
    load_angles.start()
    load_gain.start()
    load_keys.start()
    pl.semaphore_wait(barrier, 3 + 4 * core)
    pl.semaphore_signal(ready_sem, inc=1, device_id=device(0, 0, 1), device_id_type=MESH)

    def relay_out(source, relay, i):
        dx, dc = STEPS[i]
        return plan(source.at[index(dx, 1, dc)], relay.at[i], 0, 1, 0)

    def forward(relay, land, i):
        dx, dc = STEPS[i]
        return send(relay.at[i], land.at[block(across)], dx, 0, dc)

    def along_x(source, land, i, first, rows):
        dx, dc = STEPS[i]
        part = pl.ds(first, rows)
        return plan(source.at[index(dx, 0, dc), part], land.at[block(me, first, rows)], dx, 0, dc)

    def along_z(source, land, dc):
        return send(source.at[index(0, 1, dc)], land.at[block(me)], 0, 1, dc)

    def to_sibling(source, land):
        return send(source.at[index(0, 0, 1)], land.at[block(me)], 0, 0, 1)

    vz = [relay_out(values, vrelay, i) for i in range(RELAYED)]
    vx = [along_x(values, vland, i, 0, FIRST_ROWS) for i in range(RELAYED)]

    @pl.when(core == 0)
    def _():
        start(vz[:Z_FIRST])

    @pl.when(core == 1)
    def _():
        start(vx)

    pl.semaphore_wait(ready_sem, 1)

    @pl.when(core == 0)
    def _():
        start(vx)

    @pl.when(core == 1)
    def _():
        start(vz[:Z_FIRST])

    copies = vx + [to_sibling(values, vland)]
    keep.start()

    load_angles.wait()
    for c in range(ROWS // CHUNK):
        a = angles[:, c * CHUNK : (c + 1) * CHUNK]
        cosine, sine = jnp.cos(a), jnp.sin(a)
        rows = pl.ds(c * CHUNK, CHUNK)
        cosines[rows, :] = jnp.concatenate([cosine, cosine], axis=0).T
        sines[rows, :] = jnp.concatenate([-sine, sine], axis=0).T

    load_gain.wait()
    load_keys.wait()
    gains = gains_row[...]

    def turn_sequence(s, _):
        largest = jnp.zeros((8, LANES), jnp.float32)
        for c in range(ROWS // CHUNK):
            rows = pl.ds(c * CHUNK, CHUNK)
            wide = raw[s, rows, :].astype(jnp.float32)
            mean = jnp.mean(wide * wide, axis=-1, keepdims=True)
            wide = wide * lax.rsqrt(mean + 1e-06) * gains
            out = wide * cosines[rows, :] + pltpu.roll(wide, HALF, 1) * sines[rows, :]
            turned[s, rows, :] = out
            largest = jnp.maximum(
                largest, jnp.max(jnp.abs(out).reshape(CHUNK // 8, 8, LANES), axis=0)
            )
        maxes[0, pl.ds(s, 1), :] = jnp.max(largest, axis=0, keepdims=True)
        return 0

    lax.fori_loop(0, SEQS, turn_sequence, 0)

    first = send(maxes.at[0], maxes.at[1], 0, 1, 0)
    start(vz[Z_FIRST:])
    for dc in (0, 1):
        copies.append(along_z(values, vland, dc))
    if FIRST_ROWS < ROWS:
        rest = [along_x(values, vland, i, FIRST_ROWS, ROWS - FIRST_ROWS) for i in range(RELAYED)]
        start(rest)
        copies += rest
    for i in range(V_ONE):
        vz[i].wait_recv()
        copies.append(forward(vrelay, vland, i))
    first.wait()
    maxes[2] = jnp.maximum(maxes[0], maxes[1])
    second = [
        send(maxes.at[2], maxes.at[3 + i], dx, 0, dc) for i, (dx, dc) in enumerate(STEPS + [(0, 1)])
    ]
    for i in range(V_ONE, V_TWO):
        vz[i].wait_recv()
        copies.append(forward(vrelay, vland, i))
    for copy in second:
        copy.wait()
    largest = maxes[2]
    for i in range(PLANE):
        largest = jnp.maximum(largest, maxes[3 + i])
    maxes[0] = largest
    scale[...] = maxes[0, pl.ds(me, 1), :]

    def scale_sequence(s, _):
        inverse = 1.0 / maxes[0, pl.ds(s, 1), :]
        for c in range(ROWS // CHUNK):
            rows = pl.ds(c * CHUNK, CHUNK)
            narrow[s, rows, :] = (turned[s, rows, :] * inverse).astype(jnp.bfloat16)
        return 0

    lax.fori_loop(0, SEQS, scale_sequence, 0)

    kz = [relay_out(narrow, krelay, i) for i in range(RELAYED)]
    start(kz)
    for dc in (0, 1):
        copies.append(along_z(narrow, kland, dc))
    for i in range(V_TWO, RELAYED):
        vz[i].wait_recv()
        copies.append(forward(vrelay, vland, i))
    kx = [along_x(narrow, kland, i, 0, ROWS) for i in range(RELAYED)]
    start(kx)
    copies += kx
    copies.append(to_sibling(narrow, kland))

    def keep_rows(c, _):
        kland[block(me, c * CHUNK, CHUNK), :] = narrow[
            me, pl.ds(pl.multiple_of(c * CHUNK, CHUNK), CHUNK), :
        ]
        return 0

    lax.fori_loop(0, ROWS // CHUNK, keep_rows, 0)
    for i in range(RELAYED):
        kz[i].wait_recv()
        copies.append(forward(krelay, kland, i))
    keep.wait()
    for copy in vz + kz:
        copy.wait_send()
    for copy in copies:
        copy.wait()


PIECES = 2


def store(kland, vland, scale, kout, vout, scale_out, sems):
    rows = TOTAL // PIECES
    copies = []
    for i, (source, target) in enumerate(((kland, kout), (vland, vout))):
        for j in range(PIECES):
            part = pl.ds(j * rows, rows)
            copies.append(pltpu.make_async_copy(source.at[part], target.at[part], sems.at[i, j]))
    copies.append(pltpu.make_async_copy(scale, scale_out, sems.at[2, 0]))
    for copy in copies:
        copy.start()
    for copy in copies:
        copy.wait()


def local(raw_keys, raw_values, turn_angle, key_gain):
    shape = (SEQS, ROWS, LANES)
    hbm = pl.BlockSpec(memory_space=pltpu.HBM)
    vmem = pl.BlockSpec(memory_space=pltpu.VMEM)
    kland, vland, scale = pl.pallas_call(
        exchange,
        name="exchange",
        out_shape=(
            pltpu.VMEM((TOTAL, LANES), jnp.bfloat16),
            pltpu.VMEM((TOTAL, LANES), jnp.bfloat16),
            pltpu.VMEM((1, LANES), jnp.float32),
        ),
        in_specs=[hbm, hbm, hbm, hbm],
        out_specs=(vmem, vmem, vmem),
        scratch_shapes=[
            pltpu.VMEM(shape, jnp.bfloat16),
            pltpu.VMEM(shape, jnp.float32),
            pltpu.VMEM(shape, jnp.bfloat16),
            pltpu.VMEM((RELAYED, ROWS, LANES), jnp.bfloat16),
            pltpu.VMEM((RELAYED, ROWS, LANES), jnp.bfloat16),
            pltpu.VMEM((HALF, ROWS), jnp.float32),
            pltpu.VMEM((1, LANES), jnp.float32),
            pltpu.VMEM((ROWS, LANES), jnp.float32),
            pltpu.VMEM((ROWS, LANES), jnp.float32),
            pltpu.VMEM((3 + PLANE, SEQS, LANES), jnp.float32),
            pltpu.SemaphoreType.DMA((4,)),
            pltpu.SemaphoreType.REGULAR,
            pltpu.SemaphoreType.DMA((COPIES,)),
            pltpu.SemaphoreType.DMA((COPIES,)),
        ],
        compiler_params=pltpu.CompilerParams(
            collective_id=0, has_side_effects=True, vmem_limit_bytes=40 * 2**20
        ),
    )(
        *(
            pltpu.with_memory_space_constraint(array, pltpu.HBM)
            for array in (
                raw_keys.reshape(shape),
                raw_values.reshape(shape),
                turn_angle.T,
                key_gain.reshape(1, LANES),
            )
        )
    )
    kout, vout, scale = pl.pallas_call(
        store,
        name="store",
        out_shape=(
            jax.ShapeDtypeStruct((TOTAL, LANES), jnp.bfloat16),
            jax.ShapeDtypeStruct((TOTAL, LANES), jnp.bfloat16),
            jax.ShapeDtypeStruct((1, LANES), jnp.float32),
        ),
        in_specs=[vmem, vmem, vmem],
        out_specs=(hbm, hbm, hbm),
        scratch_shapes=[pltpu.SemaphoreType.DMA((3, PIECES))],
        compiler_params=pltpu.CompilerParams(vmem_limit_bytes=2**20),
    )(kland, vland, scale)
    whole = (1, TOTAL, 1, LANES)
    return kout.reshape(whole), vout.reshape(whole), scale.reshape(1, 1, LANES)


def solution(mesh):
    in_specs = (
        P(None, ("farcp", "nearcp"), "model", None),
        P(None, ("farcp", "nearcp"), "model", None),
        P(),
        P(),
    )
    out_specs = (
        P(("farcp", "nearcp"), None, "model", None),
        P(("farcp", "nearcp"), None, "model", None),
        P(("farcp", "nearcp"), "model", None),
    )
    return jax.shard_map(local, mesh=mesh, in_specs=in_specs, out_specs=out_specs, check_vma=False)
```

```python
import jax
import jax.numpy as jnp
from jax import lax
from jax.experimental import pallas as pl
from jax.experimental.pallas import tpu as pltpu
from jax.sharding import PartitionSpec as P

MESH = pl.DeviceIdType.MESH
SEQS, ROWS, LANES, HALF = 16, 1024, 128, 64
TOTAL = SEQS * ROWS
CHUNK = 128
FIRST_ROWS = 768
Z_FIRST = 3
V_ONE, V_TWO = 2, 4


ALONG_X = (1, 3, 2)
RELAYED = 2 * len(ALONG_X)
PLANE = RELAYED + 1
COPIES = 64


def exchange(
    keys, values, angle, gain,
    kland, vland, scale,
    raw, turned, narrow, krelay, vrelay, angles, gains_row, cosines, sines, maxes,
    local_sem, ready_sem, send_sem, recv_sem,
):
    far, near, model = lax.axis_index("farcp"), lax.axis_index("nearcp"), lax.axis_index("model")
    core, x, z = near % 2, ((near // 2) % 2) * 2 + far, near // 4
    used = [0]

    def place(dx, dz, dc):
        px, pz, pc = (x + dx) % 4, (z + dz) % 2, (core + dc) % 2
        return px % 2, pz * 4 + (px // 2) * 2 + pc

    def device(dx, dz, dc):
        return (*place(dx, dz, dc), model)

    def index(dx, dz, dc):
        f, n = place(dx, dz, dc)
        return f * 8 + n

    def block(owner, first=0, rows=ROWS):
        return pl.ds(pl.multiple_of(owner * ROWS + first, CHUNK), rows)

    me, across = far * 8 + near, index(0, 1, 0)

    steps = [(dx, (core + to) % 2, n) for to in (1, 0) for n, dx in enumerate(ALONG_X)]
    steps = [(dx, dc, n + len(ALONG_X) * dc) for dx, dc, n in steps]

    def plan(source, target, dx, dz, dc, slot):
        return pltpu.make_async_remote_copy(
            src_ref=source,
            dst_ref=target,
            send_sem=send_sem.at[slot],
            recv_sem=recv_sem.at[slot],
            device_id=device(dx, dz, dc),
            device_id_type=MESH,
        )

    def slots(count):
        used[0] += count
        return used[0] - count

    def start(copies):
        for copy in copies:
            copy.start()

    load_keys = pltpu.make_async_copy(keys, raw, local_sem.at[0])
    load_angles = pltpu.make_async_copy(angle.at[:, block(me)], angles, local_sem.at[1])
    load_gain = pltpu.make_async_copy(gain, gains_row, local_sem.at[2])
    keep = pltpu.make_async_copy(values.at[me], vland.at[block(me)], local_sem.at[3])

    barrier = pltpu.get_barrier_semaphore()
    greeted = [device(0, 1, core), device(0, 0, 1)] + [device(dx, 0, 1 - core) for dx in (1, 3, 2)]
    for target in greeted:
        pl.semaphore_signal(barrier, inc=1, device_id=target, device_id_type=MESH)
    load_angles.start()
    load_gain.start()
    load_keys.start()
    pl.semaphore_wait(barrier, 3 + 4 * core)
    pl.semaphore_signal(ready_sem, inc=1, device_id=device(0, 0, 1), device_id_type=MESH)

    def relay_out(source, relay):
        base = slots(RELAYED)
        return [
            plan(source.at[index(dx, 1, dc)], relay.at[i], 0, 1, 0, base + i) for dx, dc, i in steps
        ]

    def forward(relay, land):
        base = slots(RELAYED)
        return [
            plan(relay.at[i], land.at[block(across)], dx, 0, dc, base + i) for dx, dc, i in steps
        ]

    def along_x(source, land, first, rows):
        base, part = slots(RELAYED), pl.ds(first, rows)
        return [
            plan(
                source.at[index(dx, 0, dc), part],
                land.at[block(me, first, rows)],
                dx, 0, dc, base + i,
            )
            for dx, dc, i in steps
        ]

    def along_z(source, land):
        base = slots(2)
        return [
            plan(source.at[index(0, 1, dc)], land.at[block(me)], 0, 1, dc, base + dc)
            for dc in ((core + 1) % 2, core)
        ]

    def to_sibling(source, land):
        return [plan(source.at[index(0, 0, 1)], land.at[block(me)], 0, 0, 1, slots(1))]

    vz, vf = relay_out(values, vrelay), forward(vrelay, vland)
    vx = along_x(values, vland, 0, FIRST_ROWS)
    side = to_sibling(values, vland)

    @pl.when(core == 0)
    def _():
        start(vz[:Z_FIRST])

    @pl.when(core == 1)
    def _():
        start(vx)

    pl.semaphore_wait(ready_sem, 1)

    @pl.when(core == 0)
    def _():
        start(vx)

    @pl.when(core == 1)
    def _():
        start(vz[:Z_FIRST])

    start(side)
    copies = vx + vf + side
    keep.start()

    load_angles.wait()
    for c in range(ROWS // CHUNK):
        a = angles[:, c * CHUNK : (c + 1) * CHUNK]
        cosine, sine = jnp.cos(a), jnp.sin(a)
        rows = pl.ds(c * CHUNK, CHUNK)
        cosines[rows, :] = jnp.concatenate([cosine, cosine], axis=0).T
        sines[rows, :] = jnp.concatenate([-sine, sine], axis=0).T

    load_gain.wait()
    load_keys.wait()
    gains = gains_row[...]

    def turn_sequence(s, _):
        largest = jnp.zeros((8, LANES), jnp.float32)
        for c in range(ROWS // CHUNK):
            rows = pl.ds(c * CHUNK, CHUNK)
            wide = raw[s, rows, :].astype(jnp.float32)
            mean = jnp.mean(wide * wide, axis=-1, keepdims=True)
            wide = wide * lax.rsqrt(mean + 1e-06) * gains
            out = wide * cosines[rows, :] + pltpu.roll(wide, HALF, 1) * sines[rows, :]
            turned[s, rows, :] = out
            largest = jnp.maximum(
                largest, jnp.max(jnp.abs(out).reshape(CHUNK // 8, 8, LANES), axis=0)
            )
        maxes[0, pl.ds(s, 1), :] = jnp.max(largest, axis=0, keepdims=True)
        return 0

    lax.fori_loop(0, SEQS, turn_sequence, 0)

    first = plan(maxes.at[0], maxes.at[1], 0, 1, 0, slots(1))
    first.start()
    start(vz[Z_FIRST:])
    straight = along_z(values, vland)
    rest = along_x(values, vland, FIRST_ROWS, ROWS - FIRST_ROWS)
    start(straight + rest)
    copies += straight + rest
    for i in range(V_ONE):
        vz[i].wait_recv()
        vf[i].start()
    first.wait()
    maxes[2] = jnp.maximum(maxes[0], maxes[1])
    base = slots(PLANE)
    second = [
        plan(maxes.at[2], maxes.at[3 + i], dx, 0, dc, base + i)
        for dx, dc, i in steps + [(0, 1, RELAYED)]
    ]
    start(second)
    for i in range(V_ONE, V_TWO):
        vz[i].wait_recv()
        vf[i].start()
    for copy in second:
        copy.wait()
    largest = maxes[2]
    for i in range(PLANE):
        largest = jnp.maximum(largest, maxes[3 + i])
    maxes[0] = largest
    scale[...] = maxes[0, pl.ds(me, 1), :]

    def scale_sequence(s, _):
        inverse = 1.0 / maxes[0, pl.ds(s, 1), :]
        for c in range(ROWS // CHUNK):
            rows = pl.ds(c * CHUNK, CHUNK)
            narrow[s, rows, :] = (turned[s, rows, :] * inverse).astype(jnp.bfloat16)
        return 0

    lax.fori_loop(0, SEQS, scale_sequence, 0)

    kz, kf = relay_out(narrow, krelay), forward(krelay, kland)
    straight = along_z(narrow, kland)
    start(kz + straight)
    for i in range(V_TWO, RELAYED):
        vz[i].wait_recv()
        vf[i].start()
    kx = along_x(narrow, kland, 0, ROWS) + to_sibling(narrow, kland)
    start(kx)
    copies += straight + kx + kf

    def keep_rows(c, _):
        kland[block(me, c * CHUNK, CHUNK), :] = narrow[
            me, pl.ds(pl.multiple_of(c * CHUNK, CHUNK), CHUNK), :
        ]
        return 0

    lax.fori_loop(0, ROWS // CHUNK, keep_rows, 0)
    for i in range(RELAYED):
        kz[i].wait_recv()
        kf[i].start()
    keep.wait()
    for copy in vz + kz:
        copy.wait_send()
    for copy in copies:
        copy.wait()


PIECES = 2


def store(kland, vland, scale, kout, vout, scale_out, sems):
    rows = TOTAL // PIECES
    copies = []
    for i, (source, target) in enumerate(((kland, kout), (vland, vout))):
        for j in range(PIECES):
            part = pl.ds(j * rows, rows)
            copies.append(pltpu.make_async_copy(source.at[part], target.at[part], sems.at[i, j]))
    copies.append(pltpu.make_async_copy(scale, scale_out, sems.at[2, 0]))
    for copy in copies:
        copy.start()
    for copy in copies:
        copy.wait()


def local(raw_keys, raw_values, turn_angle, key_gain):
    shape = (SEQS, ROWS, LANES)
    hbm = pl.BlockSpec(memory_space=pltpu.HBM)
    vmem = pl.BlockSpec(memory_space=pltpu.VMEM)
    kland, vland, scale = pl.pallas_call(
        exchange,
        name="exchange",
        out_shape=(
            pltpu.VMEM((TOTAL, LANES), jnp.bfloat16),
            pltpu.VMEM((TOTAL, LANES), jnp.bfloat16),
            pltpu.VMEM((1, LANES), jnp.float32),
        ),
        in_specs=[hbm, hbm, hbm, hbm],
        out_specs=(vmem, vmem, vmem),
        scratch_shapes=[
            pltpu.VMEM(shape, jnp.bfloat16),
            pltpu.VMEM(shape, jnp.float32),
            pltpu.VMEM(shape, jnp.bfloat16),
            pltpu.VMEM((RELAYED, ROWS, LANES), jnp.bfloat16),
            pltpu.VMEM((RELAYED, ROWS, LANES), jnp.bfloat16),
            pltpu.VMEM((HALF, ROWS), jnp.float32),
            pltpu.VMEM((1, LANES), jnp.float32),
            pltpu.VMEM((ROWS, LANES), jnp.float32),
            pltpu.VMEM((ROWS, LANES), jnp.float32),
            pltpu.VMEM((3 + PLANE, SEQS, LANES), jnp.float32),
            pltpu.SemaphoreType.DMA((4,)),
            pltpu.SemaphoreType.REGULAR,
            pltpu.SemaphoreType.DMA((COPIES,)),
            pltpu.SemaphoreType.DMA((COPIES,)),
        ],
        compiler_params=pltpu.CompilerParams(
            collective_id=0, has_side_effects=True, vmem_limit_bytes=40 * 2**20
        ),
    )(
        *(
            pltpu.with_memory_space_constraint(array, pltpu.HBM)
            for array in (
                raw_keys.reshape(shape),
                raw_values.reshape(shape),
                turn_angle.T,
                key_gain.reshape(1, LANES),
            )
        )
    )
    kout, vout, scale = pl.pallas_call(
        store,
        name="store",
        out_shape=(
            jax.ShapeDtypeStruct((TOTAL, LANES), jnp.bfloat16),
            jax.ShapeDtypeStruct((TOTAL, LANES), jnp.bfloat16),
            jax.ShapeDtypeStruct((1, LANES), jnp.float32),
        ),
        in_specs=[vmem, vmem, vmem],
        out_specs=(hbm, hbm, hbm),
        scratch_shapes=[pltpu.SemaphoreType.DMA((3, PIECES))],
        compiler_params=pltpu.CompilerParams(vmem_limit_bytes=2**20),
    )(kland, vland, scale)
    whole = (1, TOTAL, 1, LANES)
    return kout.reshape(whole), vout.reshape(whole), scale.reshape(1, 1, LANES)


def solution(mesh):
    in_specs = (
        P(None, ("farcp", "nearcp"), "model", None),
        P(None, ("farcp", "nearcp"), "model", None),
        P(),
        P(),
    )
    out_specs = (
        P(("farcp", "nearcp"), None, "model", None),
        P(("farcp", "nearcp"), None, "model", None),
        P(("farcp", "nearcp"), "model", None),
    )
    return jax.shard_map(local, mesh=mesh, in_specs=in_specs, out_specs=out_specs, check_vma=False)
```

```python
import jax
import jax.numpy as jnp
from jax import lax
from jax.experimental import pallas as pl
from jax.experimental.pallas import tpu as pltpu
from jax.sharding import PartitionSpec as P

MESH = pl.DeviceIdType.MESH
SEQS, ROWS, LANES, HALF = 16, 1024, 128, 64
TOTAL = SEQS * ROWS
CHUNK = 128
FIRST_ROWS = 768
Z_FIRST = 3
V_ONE, V_TWO = 2, 4


ALONG_X = (1, 3, 2)
RELAYED = 2 * len(ALONG_X)
PLANE = RELAYED + 1
ARRIVING = 15 * ROWS


def exchange(
    keys, values, angle, gain,
    kland, vland, scale,
    raw, turned, narrow, krelay, vrelay, angles, gains_row, cosines, sines, maxes,
    local_sem, ready_sem, send_sem, land_sem, hop_sem, max_sem,
):
    far, near, model = lax.axis_index("farcp"), lax.axis_index("nearcp"), lax.axis_index("model")
    core, x, z = near % 2, ((near // 2) % 2) * 2 + far, near // 4

    def place(dx, dz, dc):
        px, pz, pc = (x + dx) % 4, (z + dz) % 2, (core + dc) % 2
        return px % 2, pz * 4 + (px // 2) * 2 + pc

    def device(dx, dz, dc):
        return (*place(dx, dz, dc), model)

    def index(dx, dz, dc):
        f, n = place(dx, dz, dc)
        return f * 8 + n

    def block(owner, first=0, rows=ROWS):
        return pl.ds(pl.multiple_of(owner * ROWS + first, CHUNK), rows)

    me, across = far * 8 + near, index(0, 1, 0)

    steps = [(dx, (core + to) % 2, n) for to in (1, 0) for n, dx in enumerate(ALONG_X)]
    steps = [(dx, dc, n + len(ALONG_X) * dc) for dx, dc, n in steps]

    def plan(source, target, dx, dz, dc, sent, arrived):
        return pltpu.make_async_remote_copy(
            src_ref=source,
            dst_ref=target,
            send_sem=sent,
            recv_sem=arrived,
            device_id=device(dx, dz, dc),
            device_id_type=MESH,
        )

    def wait_for(ref, sem):
        pltpu.make_async_copy(ref, ref, sem).wait()

    def start(copies):
        for copy in copies:
            copy.start()

    load_keys = pltpu.make_async_copy(keys, raw, local_sem.at[0])
    load_angles = pltpu.make_async_copy(angle.at[:, block(me)], angles, local_sem.at[1])
    load_gain = pltpu.make_async_copy(gain, gains_row, local_sem.at[2])
    keep = pltpu.make_async_copy(values.at[me], vland.at[block(me)], local_sem.at[3])

    barrier = pltpu.get_barrier_semaphore()
    greeted = [device(0, 1, core), device(0, 0, 1)] + [device(dx, 0, 1 - core) for dx in (1, 3, 2)]
    for target in greeted:
        pl.semaphore_signal(barrier, inc=1, device_id=target, device_id_type=MESH)
    load_angles.start()
    load_gain.start()
    load_keys.start()
    pl.semaphore_wait(barrier, 3 + 4 * core)
    pl.semaphore_signal(ready_sem, inc=1, device_id=device(0, 0, 1), device_id_type=MESH)

    def relay_out(n, source, relay):
        return [
            plan(
                source.at[index(dx, 1, dc)], relay.at[i],
                0, 1, 0, send_sem.at[n], hop_sem.at[n, i],
            )
            for dx, dc, i in steps
        ]

    def forward(n, relay, land):
        return [
            plan(
                relay.at[i], land.at[block(across)],
                dx, 0, dc, send_sem.at[2 + n], land_sem.at[n],
            )
            for dx, dc, i in steps
        ]

    def along_x(n, source, land, first, rows):
        part = pl.ds(first, rows)
        return [
            plan(
                source.at[index(dx, 0, dc), part], land.at[block(me, first, rows)],
                dx, 0, dc, send_sem.at[2 + n], land_sem.at[n],
            )
            for dx, dc, i in steps
        ]

    def straight(n, source, land, dz, dc):
        return plan(
            source.at[index(0, dz, dc)], land.at[block(me)],
            0, dz, dc, send_sem.at[2 + n], land_sem.at[n],
        )

    def along_z(n, source, land):
        return [straight(n, source, land, 1, dc) for dc in ((core + 1) % 2, core)]

    def to_sibling(n, source, land):
        return [straight(n, source, land, 0, 1)]

    vz, vf = relay_out(0, values, vrelay), forward(0, vrelay, vland)
    vx = along_x(0, values, vland, 0, FIRST_ROWS)

    @pl.when(core == 0)
    def _():
        start(vz[:Z_FIRST])

    @pl.when(core == 1)
    def _():
        start(vx)

    pl.semaphore_wait(ready_sem, 1)

    @pl.when(core == 0)
    def _():
        start(vx)

    @pl.when(core == 1)
    def _():
        start(vz[:Z_FIRST])

    start(to_sibling(0, values, vland))
    keep.start()

    load_angles.wait()
    for c in range(ROWS // CHUNK):
        a = angles[:, c * CHUNK : (c + 1) * CHUNK]
        cosine, sine = jnp.cos(a), jnp.sin(a)
        rows = pl.ds(c * CHUNK, CHUNK)
        cosines[rows, :] = jnp.concatenate([cosine, cosine], axis=0).T
        sines[rows, :] = jnp.concatenate([-sine, sine], axis=0).T

    load_gain.wait()
    load_keys.wait()
    gains = gains_row[...]

    def turn_sequence(s, _):
        largest = jnp.zeros((8, LANES), jnp.float32)
        for c in range(ROWS // CHUNK):
            rows = pl.ds(c * CHUNK, CHUNK)
            wide = raw[s, rows, :].astype(jnp.float32)
            mean = jnp.mean(wide * wide, axis=-1, keepdims=True)
            wide = wide * lax.rsqrt(mean + 1e-06) * gains
            out = wide * cosines[rows, :] + pltpu.roll(wide, HALF, 1) * sines[rows, :]
            turned[s, rows, :] = out
            largest = jnp.maximum(
                largest, jnp.max(jnp.abs(out).reshape(CHUNK // 8, 8, LANES), axis=0)
            )
        maxes[0, pl.ds(s, 1), :] = jnp.max(largest, axis=0, keepdims=True)
        return 0

    lax.fori_loop(0, SEQS, turn_sequence, 0)

    first = plan(maxes.at[0], maxes.at[1], 0, 1, 0, max_sem.at[0], max_sem.at[1])
    first.start()
    start(vz[Z_FIRST:])
    start(along_z(0, values, vland))
    start(along_x(0, values, vland, FIRST_ROWS, ROWS - FIRST_ROWS))
    for i in range(V_ONE):
        vz[i].wait_recv()
        vf[i].start()
    first.wait()
    maxes[2] = jnp.maximum(maxes[0], maxes[1])
    second = [
        plan(maxes.at[2], maxes.at[3 + i], dx, 0, dc, max_sem.at[2], max_sem.at[3])
        for dx, dc, i in steps + [(0, 1, RELAYED)]
    ]
    start(second)
    for i in range(V_ONE, V_TWO):
        vz[i].wait_recv()
        vf[i].start()
    wait_for(maxes.at[pl.ds(3, PLANE)], max_sem.at[3])
    largest = maxes[2]
    for i in range(PLANE):
        largest = jnp.maximum(largest, maxes[3 + i])
    maxes[0] = largest
    scale[...] = maxes[0, pl.ds(me, 1), :]

    def scale_sequence(s, _):
        inverse = 1.0 / maxes[0, pl.ds(s, 1), :]
        for c in range(ROWS // CHUNK):
            rows = pl.ds(c * CHUNK, CHUNK)
            narrow[s, rows, :] = (turned[s, rows, :] * inverse).astype(jnp.bfloat16)
        return 0

    lax.fori_loop(0, SEQS, scale_sequence, 0)

    kz, kf = relay_out(1, narrow, krelay), forward(1, krelay, kland)
    start(kz + along_z(1, narrow, kland))
    for i in range(V_TWO, RELAYED):
        vz[i].wait_recv()
        vf[i].start()
    start(along_x(1, narrow, kland, 0, ROWS) + to_sibling(1, narrow, kland))

    def keep_rows(c, _):
        kland[block(me, c * CHUNK, CHUNK), :] = narrow[
            me, pl.ds(pl.multiple_of(c * CHUNK, CHUNK), CHUNK), :
        ]
        return 0

    lax.fori_loop(0, ROWS // CHUNK, keep_rows, 0)
    for i in range(RELAYED):
        kz[i].wait_recv()
        kf[i].start()
    keep.wait()
    wait_for(maxes.at[pl.ds(3, PLANE)], max_sem.at[2])
    for n, (relay, land) in enumerate(((vrelay, vland), (krelay, kland))):
        arriving = land.at[pl.ds(0, ARRIVING)]
        wait_for(relay, send_sem.at[n])
        wait_for(arriving, send_sem.at[2 + n])
        wait_for(arriving, land_sem.at[n])


PIECES = 2


def store(kland, vland, scale, kout, vout, scale_out, sems):
    rows = TOTAL // PIECES
    copies = []
    for i, (source, target) in enumerate(((kland, kout), (vland, vout))):
        for j in range(PIECES):
            part = pl.ds(j * rows, rows)
            copies.append(pltpu.make_async_copy(source.at[part], target.at[part], sems.at[i, j]))
    copies.append(pltpu.make_async_copy(scale, scale_out, sems.at[2, 0]))
    for copy in copies:
        copy.start()
    for copy in copies:
        copy.wait()


def local(raw_keys, raw_values, turn_angle, key_gain):
    shape = (SEQS, ROWS, LANES)
    hbm = pl.BlockSpec(memory_space=pltpu.HBM)
    vmem = pl.BlockSpec(memory_space=pltpu.VMEM)
    kland, vland, scale = pl.pallas_call(
        exchange,
        name="exchange",
        out_shape=(
            pltpu.VMEM((TOTAL, LANES), jnp.bfloat16),
            pltpu.VMEM((TOTAL, LANES), jnp.bfloat16),
            pltpu.VMEM((1, LANES), jnp.float32),
        ),
        in_specs=[hbm, hbm, hbm, hbm],
        out_specs=(vmem, vmem, vmem),
        scratch_shapes=[
            pltpu.VMEM(shape, jnp.bfloat16),
            pltpu.VMEM(shape, jnp.float32),
            pltpu.VMEM(shape, jnp.bfloat16),
            pltpu.VMEM((RELAYED, ROWS, LANES), jnp.bfloat16),
            pltpu.VMEM((RELAYED, ROWS, LANES), jnp.bfloat16),
            pltpu.VMEM((HALF, ROWS), jnp.float32),
            pltpu.VMEM((1, LANES), jnp.float32),
            pltpu.VMEM((ROWS, LANES), jnp.float32),
            pltpu.VMEM((ROWS, LANES), jnp.float32),
            pltpu.VMEM((3 + PLANE, SEQS, LANES), jnp.float32),
            pltpu.SemaphoreType.DMA((4,)),
            pltpu.SemaphoreType.REGULAR,
            pltpu.SemaphoreType.DMA((4,)),
            pltpu.SemaphoreType.DMA((2,)),
            pltpu.SemaphoreType.DMA((2, RELAYED)),
            pltpu.SemaphoreType.DMA((4,)),
        ],
        compiler_params=pltpu.CompilerParams(
            collective_id=0, has_side_effects=True, vmem_limit_bytes=40 * 2**20
        ),
    )(
        *(
            pltpu.with_memory_space_constraint(array, pltpu.HBM)
            for array in (
                raw_keys.reshape(shape),
                raw_values.reshape(shape),
                turn_angle.T,
                key_gain.reshape(1, LANES),
            )
        )
    )
    kout, vout, scale = pl.pallas_call(
        store,
        name="store",
        out_shape=(
            jax.ShapeDtypeStruct((TOTAL, LANES), jnp.bfloat16),
            jax.ShapeDtypeStruct((TOTAL, LANES), jnp.bfloat16),
            jax.ShapeDtypeStruct((1, LANES), jnp.float32),
        ),
        in_specs=[vmem, vmem, vmem],
        out_specs=(hbm, hbm, hbm),
        scratch_shapes=[pltpu.SemaphoreType.DMA((3, PIECES))],
        compiler_params=pltpu.CompilerParams(vmem_limit_bytes=2**20),
    )(kland, vland, scale)
    whole = (1, TOTAL, 1, LANES)
    return kout.reshape(whole), vout.reshape(whole), scale.reshape(1, 1, LANES)


def solution(mesh):
    in_specs = (
        P(None, ("farcp", "nearcp"), "model", None),
        P(None, ("farcp", "nearcp"), "model", None),
        P(),
        P(),
    )
    out_specs = (
        P(("farcp", "nearcp"), None, "model", None),
        P(("farcp", "nearcp"), None, "model", None),
        P(("farcp", "nearcp"), "model", None),
    )
    return jax.shard_map(local, mesh=mesh, in_specs=in_specs, out_specs=out_specs, check_vma=False)
```

```python
import jax
import jax.numpy as jnp
from jax import lax
from jax.experimental import pallas as pl
from jax.experimental.pallas import tpu as pltpu
from jax.sharding import PartitionSpec as P

MESH = pl.DeviceIdType.MESH
SEQS, ROWS, LANES, HALF = 16, 1024, 128, 64
TOTAL = SEQS * ROWS
CHUNK = 128
FIRST_ROWS = 896
Z_FIRST = 4
V_ONE, V_TWO = 3, 6


ALONG_X = (1, 3, 2)
RELAYED = 2 * len(ALONG_X)
PLANE = RELAYED + 1
ARRIVING = 15 * ROWS


def exchange(
    keys, values, angle, gain,
    kland, vland, scale,
    raw, turned, narrow, krelay, vrelay, angles, gains_row, cosines, sines, maxes,
    local_sem, ready_sem, send_sem, land_sem, hop_sem, max_sem,
):
    far, near, model = lax.axis_index("farcp"), lax.axis_index("nearcp"), lax.axis_index("model")
    core, x, z = lax.rem(near, 2), lax.rem(lax.div(near, 2), 2) * 2 + far, lax.div(near, 4)

    def place(dx, dz, dc):
        px, pz, pc = lax.rem(x + dx, 4), lax.rem(z + dz, 2), lax.rem(core + dc, 2)
        return lax.rem(px, 2), pz * 4 + lax.div(px, 2) * 2 + pc

    def device(dx, dz, dc):
        return (*place(dx, dz, dc), model)

    def index(dx, dz, dc):
        f, n = place(dx, dz, dc)
        return f * 8 + n

    def block(owner, first=0, rows=ROWS):
        return pl.ds(pl.multiple_of(owner * ROWS + first, CHUNK), rows)

    me, across = far * 8 + near, index(0, 1, 0)

    steps = [(dx, lax.rem(core + to, 2), n) for to in (1, 0) for n, dx in enumerate(ALONG_X)]
    steps = [(dx, dc, n + len(ALONG_X) * dc) for dx, dc, n in steps]

    def plan(source, target, dx, dz, dc, sent, arrived):
        return pltpu.make_async_remote_copy(
            src_ref=source,
            dst_ref=target,
            send_sem=sent,
            recv_sem=arrived,
            device_id=device(dx, dz, dc),
            device_id_type=MESH,
        )

    def wait_for(ref, sem):
        pltpu.make_async_copy(ref, ref, sem).wait()

    def start(copies):
        for copy in copies:
            copy.start()

    load_keys = pltpu.make_async_copy(keys, raw, local_sem.at[0])
    load_angles = pltpu.make_async_copy(angle.at[:, block(me)], angles, local_sem.at[1])
    load_gain = pltpu.make_async_copy(gain, gains_row, local_sem.at[2])
    keep = pltpu.make_async_copy(values.at[me], vland.at[block(me)], local_sem.at[3])

    barrier = pltpu.get_barrier_semaphore()
    greeted = [device(0, 1, core), device(0, 0, 1)] + [device(dx, 0, 1 - core) for dx in (1, 3, 2)]
    for target in greeted:
        pl.semaphore_signal(barrier, inc=1, device_id=target, device_id_type=MESH)
    load_angles.start()
    load_gain.start()
    load_keys.start()
    pl.semaphore_wait(barrier, 3 + 4 * core)
    pl.semaphore_signal(ready_sem, inc=1, device_id=device(0, 0, 1), device_id_type=MESH)

    def relay_out(n, source, relay):
        return [
            plan(
                source.at[index(dx, 1, dc)], relay.at[i],
                0, 1, 0, send_sem.at[n], hop_sem.at[n, i],
            )
            for dx, dc, i in steps
        ]

    def forward(n, relay, land):
        return [
            plan(
                relay.at[i], land.at[block(across)],
                dx, 0, dc, send_sem.at[2 + n], land_sem.at[n],
            )
            for dx, dc, i in steps
        ]

    def along_x(n, source, land, first, rows):
        part = pl.ds(first, rows)
        return [
            plan(
                source.at[index(dx, 0, dc), part], land.at[block(me, first, rows)],
                dx, 0, dc, send_sem.at[2 + n], land_sem.at[n],
            )
            for dx, dc, i in steps
        ]

    def straight(n, source, land, dz, dc):
        return plan(
            source.at[index(0, dz, dc)], land.at[block(me)],
            0, dz, dc, send_sem.at[2 + n], land_sem.at[n],
        )

    def along_z(n, source, land):
        return [straight(n, source, land, 1, dc) for dc in (1 - core, core)]

    def to_sibling(n, source, land):
        return [straight(n, source, land, 0, 1)]

    vz, vf = relay_out(0, values, vrelay), forward(0, vrelay, vland)
    vx = along_x(0, values, vland, 0, FIRST_ROWS)

    @pl.when(core == 0)
    def _():
        start(vz[:Z_FIRST])

    @pl.when(core == 1)
    def _():
        start(vx)

    pl.semaphore_wait(ready_sem, 1)

    @pl.when(core == 0)
    def _():
        start(vx)

    @pl.when(core == 1)
    def _():
        start(vz[:Z_FIRST])

    start(to_sibling(0, values, vland))
    keep.start()

    load_angles.wait()
    for c in range(ROWS // CHUNK):
        a = angles[:, c * CHUNK : (c + 1) * CHUNK]
        cosine, sine = jnp.cos(a), jnp.sin(a)
        rows = pl.ds(c * CHUNK, CHUNK)
        cosines[rows, :] = jnp.concatenate([cosine, cosine], axis=0).T
        sines[rows, :] = jnp.concatenate([-sine, sine], axis=0).T

    load_gain.wait()
    load_keys.wait()
    gains = gains_row[...]

    def turn_sequence(s, _):
        largest = jnp.zeros((8, LANES), jnp.float32)
        for c in range(ROWS // CHUNK):
            rows = pl.ds(c * CHUNK, CHUNK)
            wide = raw[s, rows, :].astype(jnp.float32)
            mean = jnp.mean(wide * wide, axis=-1, keepdims=True)
            wide = wide * lax.rsqrt(mean + 1e-06) * gains
            out = wide * cosines[rows, :] + pltpu.roll(wide, HALF, 1) * sines[rows, :]
            turned[s, rows, :] = out
            largest = jnp.maximum(
                largest, jnp.max(jnp.abs(out).reshape(CHUNK // 8, 8, LANES), axis=0)
            )
        maxes[0, pl.ds(s, 1), :] = jnp.max(largest, axis=0, keepdims=True)
        return 0

    lax.fori_loop(0, SEQS, turn_sequence, 0)

    first = plan(maxes.at[0], maxes.at[1], 0, 1, 0, max_sem.at[0], max_sem.at[1])
    first.start()
    start(vz[Z_FIRST:])
    start(along_z(0, values, vland))
    start(along_x(0, values, vland, FIRST_ROWS, ROWS - FIRST_ROWS))
    for i in range(V_ONE):
        vz[i].wait_recv()
        vf[i].start()
    first.wait()
    maxes[2] = jnp.maximum(maxes[0], maxes[1])
    second = [
        plan(maxes.at[2], maxes.at[3 + i], dx, 0, dc, max_sem.at[2], max_sem.at[3])
        for dx, dc, i in steps + [(0, 1, RELAYED)]
    ]
    start(second)
    for i in range(V_ONE, V_TWO):
        vz[i].wait_recv()
        vf[i].start()
    wait_for(maxes.at[pl.ds(3, PLANE)], max_sem.at[3])
    largest = maxes[2]
    for i in range(PLANE):
        largest = jnp.maximum(largest, maxes[3 + i])
    maxes[0] = largest
    scale[...] = maxes[0, pl.ds(me, 1), :]

    def scale_sequence(s, _):
        inverse = 1.0 / maxes[0, pl.ds(s, 1), :]
        for c in range(ROWS // CHUNK):
            rows = pl.ds(c * CHUNK, CHUNK)
            narrow[s, rows, :] = (turned[s, rows, :] * inverse).astype(jnp.bfloat16)
        return 0

    lax.fori_loop(0, SEQS, scale_sequence, 0)

    kz, kf = relay_out(1, narrow, krelay), forward(1, krelay, kland)
    start(kz + along_z(1, narrow, kland))
    for i in range(V_TWO, RELAYED):
        vz[i].wait_recv()
        vf[i].start()
    start(along_x(1, narrow, kland, 0, ROWS) + to_sibling(1, narrow, kland))

    def keep_rows(c, _):
        kland[block(me, c * CHUNK, CHUNK), :] = narrow[
            me, pl.ds(pl.multiple_of(c * CHUNK, CHUNK), CHUNK), :
        ]
        return 0

    lax.fori_loop(0, ROWS // CHUNK, keep_rows, 0)
    for i in range(RELAYED):
        kz[i].wait_recv()
        kf[i].start()
    keep.wait()
    wait_for(maxes.at[pl.ds(3, PLANE)], max_sem.at[2])
    for n, (relay, land) in enumerate(((vrelay, vland), (krelay, kland))):
        arriving = land.at[pl.ds(0, ARRIVING)]
        wait_for(relay, send_sem.at[n])
        wait_for(arriving, send_sem.at[2 + n])
        wait_for(arriving, land_sem.at[n])


PIECES = 2


def store(kland, vland, scale, kout, vout, scale_out, sems):
    rows = TOTAL // PIECES
    copies = []
    for i, (source, target) in enumerate(((kland, kout), (vland, vout))):
        for j in range(PIECES):
            part = pl.ds(j * rows, rows)
            copies.append(pltpu.make_async_copy(source.at[part], target.at[part], sems.at[i, j]))
    copies.append(pltpu.make_async_copy(scale, scale_out, sems.at[2, 0]))
    for copy in copies:
        copy.start()
    for copy in copies:
        copy.wait()


def local(raw_keys, raw_values, turn_angle, key_gain):
    shape = (SEQS, ROWS, LANES)
    hbm = pl.BlockSpec(memory_space=pltpu.HBM)
    vmem = pl.BlockSpec(memory_space=pltpu.VMEM)
    kland, vland, scale = pl.pallas_call(
        exchange,
        name="exchange",
        out_shape=(
            pltpu.VMEM((TOTAL, LANES), jnp.bfloat16),
            pltpu.VMEM((TOTAL, LANES), jnp.bfloat16),
            pltpu.VMEM((1, LANES), jnp.float32),
        ),
        in_specs=[hbm, hbm, hbm, hbm],
        out_specs=(vmem, vmem, vmem),
        scratch_shapes=[
            pltpu.VMEM(shape, jnp.bfloat16),
            pltpu.VMEM(shape, jnp.float32),
            pltpu.VMEM(shape, jnp.bfloat16),
            pltpu.VMEM((RELAYED, ROWS, LANES), jnp.bfloat16),
            pltpu.VMEM((RELAYED, ROWS, LANES), jnp.bfloat16),
            pltpu.VMEM((HALF, ROWS), jnp.float32),
            pltpu.VMEM((1, LANES), jnp.float32),
            pltpu.VMEM((ROWS, LANES), jnp.float32),
            pltpu.VMEM((ROWS, LANES), jnp.float32),
            pltpu.VMEM((3 + PLANE, SEQS, LANES), jnp.float32),
            pltpu.SemaphoreType.DMA((4,)),
            pltpu.SemaphoreType.REGULAR,
            pltpu.SemaphoreType.DMA((4,)),
            pltpu.SemaphoreType.DMA((2,)),
            pltpu.SemaphoreType.DMA((2, RELAYED)),
            pltpu.SemaphoreType.DMA((4,)),
        ],
        compiler_params=pltpu.CompilerParams(
            collective_id=0, has_side_effects=True, vmem_limit_bytes=40 * 2**20
        ),
    )(
        *(
            pltpu.with_memory_space_constraint(array, pltpu.HBM)
            for array in (
                raw_keys.reshape(shape),
                raw_values.reshape(shape),
                turn_angle.T,
                key_gain.reshape(1, LANES),
            )
        )
    )
    kout, vout, scale = pl.pallas_call(
        store,
        name="store",
        out_shape=(
            jax.ShapeDtypeStruct((TOTAL, LANES), jnp.bfloat16),
            jax.ShapeDtypeStruct((TOTAL, LANES), jnp.bfloat16),
            jax.ShapeDtypeStruct((1, LANES), jnp.float32),
        ),
        in_specs=[vmem, vmem, vmem],
        out_specs=(hbm, hbm, hbm),
        scratch_shapes=[pltpu.SemaphoreType.DMA((3, PIECES))],
        compiler_params=pltpu.CompilerParams(vmem_limit_bytes=2**20),
    )(kland, vland, scale)
    whole = (1, TOTAL, 1, LANES)
    return kout.reshape(whole), vout.reshape(whole), scale.reshape(1, 1, LANES)


def solution(mesh):
    in_specs = (
        P(None, ("farcp", "nearcp"), "model", None),
        P(None, ("farcp", "nearcp"), "model", None),
        P(),
        P(),
    )
    out_specs = (
        P(("farcp", "nearcp"), None, "model", None),
        P(("farcp", "nearcp"), None, "model", None),
        P(("farcp", "nearcp"), "model", None),
    )
    return jax.shard_map(local, mesh=mesh, in_specs=in_specs, out_specs=out_specs, check_vma=False)
```

```python
import jax
import jax.numpy as jnp
from jax import lax
from jax.experimental import pallas as pl
from jax.experimental.pallas import tpu as pltpu
from jax.sharding import PartitionSpec as P

MESH = pl.DeviceIdType.MESH
SEQS, ROWS, LANES, HALF = 16, 1024, 128, 64
TOTAL = SEQS * ROWS
CHUNK = 128
FIRST_ROWS = 896
Z_FIRST = 4
V_ONE, V_TWO = 3, 6


ALONG_X = (1, 3, 2)
RELAYED = 2 * len(ALONG_X)
PLANE = RELAYED + 1
ARRIVING = 15 * ROWS


def exchange(
    keys, values, angle, gain,
    kland, vland, scale,
    raw, turned, narrow, krelay, vrelay, angles, gains_row, cosines, sines, maxes,
    local_sem, ready_sem, send_sem, land_sem, hop_sem, max_sem,
):
    far, near, model = lax.axis_index("farcp"), lax.axis_index("nearcp"), lax.axis_index("model")
    core, x, z = lax.rem(near, 2), lax.rem(lax.div(near, 2), 2) * 2 + far, lax.div(near, 4)

    def place(dx, dz, dc):
        px, pz, pc = lax.rem(x + dx, 4), lax.rem(z + dz, 2), lax.rem(core + dc, 2)
        return lax.rem(px, 2), pz * 4 + lax.div(px, 2) * 2 + pc

    def device(dx, dz, dc):
        return (*place(dx, dz, dc), model)

    def index(dx, dz, dc):
        f, n = place(dx, dz, dc)
        return f * 8 + n

    def block(owner, first=0, rows=ROWS):
        return pl.ds(pl.multiple_of(owner * ROWS + first, CHUNK), rows)

    me, across = far * 8 + near, index(0, 1, 0)

    steps = [(dx, lax.rem(core + to, 2), n) for to in (1, 0) for n, dx in enumerate(ALONG_X)]
    steps = [(dx, dc, n + len(ALONG_X) * dc) for dx, dc, n in steps]

    def plan(source, target, dx, dz, dc, sent, arrived):
        return pltpu.make_async_remote_copy(
            src_ref=source,
            dst_ref=target,
            send_sem=sent,
            recv_sem=arrived,
            device_id=device(dx, dz, dc),
            device_id_type=MESH,
        )

    def wait_for(ref, sem):
        pltpu.make_async_copy(ref, ref, sem).wait()

    def start(copies):
        for copy in copies:
            copy.start()

    load_keys = pltpu.make_async_copy(keys, raw, local_sem.at[0])
    load_angles = pltpu.make_async_copy(angle.at[:, block(me)], angles, local_sem.at[1])
    load_gain = pltpu.make_async_copy(gain, gains_row, local_sem.at[2])
    keep = pltpu.make_async_copy(values.at[me], vland.at[block(me)], local_sem.at[3])

    barrier = pltpu.get_barrier_semaphore()
    greeted = [device(0, 1, core), device(0, 0, 1)] + [device(dx, 0, 1 - core) for dx in (1, 3, 2)]
    for target in greeted:
        pl.semaphore_signal(barrier, inc=1, device_id=target, device_id_type=MESH)
    load_angles.start()
    load_gain.start()
    load_keys.start()
    pl.semaphore_wait(barrier, 3 + 4 * core)
    pl.semaphore_signal(ready_sem, inc=1, device_id=device(0, 0, 1), device_id_type=MESH)

    def relay_out(n, source, relay):
        return [
            plan(
                source.at[index(dx, 1, dc)], relay.at[i],
                0, 1, 0, send_sem.at[0], hop_sem.at[n, i],
            )
            for dx, dc, i in steps
        ]

    def forward(n, relay, land):
        return [
            plan(
                relay.at[i], land.at[block(across)],
                dx, 0, dc, send_sem.at[1], land_sem.at[0],
            )
            for dx, dc, i in steps
        ]

    def along_x(n, source, land, first, rows):
        part = pl.ds(first, rows)
        return [
            plan(
                source.at[index(dx, 0, dc), part], land.at[block(me, first, rows)],
                dx, 0, dc, send_sem.at[1], land_sem.at[0],
            )
            for dx, dc, i in steps
        ]

    def straight(n, source, land, dz, dc):
        return plan(
            source.at[index(0, dz, dc)], land.at[block(me)],
            0, dz, dc, send_sem.at[1], land_sem.at[0],
        )

    def along_z(n, source, land):
        return [straight(n, source, land, 1, dc) for dc in (1 - core, core)]

    def to_sibling(n, source, land):
        return [straight(n, source, land, 0, 1)]

    vz, vf = relay_out(0, values, vrelay), forward(0, vrelay, vland)
    vx = along_x(0, values, vland, 0, FIRST_ROWS)

    @pl.when(core == 0)
    def _():
        start(vz[:Z_FIRST])

    @pl.when(core == 1)
    def _():
        start(vx)

    pl.semaphore_wait(ready_sem, 1)

    @pl.when(core == 0)
    def _():
        start(vx)

    @pl.when(core == 1)
    def _():
        start(vz[:Z_FIRST])

    start(to_sibling(0, values, vland))
    keep.start()

    load_angles.wait()
    for c in range(ROWS // CHUNK):
        a = angles[:, c * CHUNK : (c + 1) * CHUNK]
        cosine, sine = jnp.cos(a), jnp.sin(a)
        rows = pl.ds(c * CHUNK, CHUNK)
        cosines[rows, :] = jnp.concatenate([cosine, cosine], axis=0).T
        sines[rows, :] = jnp.concatenate([-sine, sine], axis=0).T

    load_gain.wait()
    load_keys.wait()
    gains = gains_row[...]

    def turn_sequence(s, _):
        largest = jnp.zeros((8, LANES), jnp.float32)
        for c in range(ROWS // CHUNK):
            rows = pl.ds(c * CHUNK, CHUNK)
            wide = raw[s, rows, :].astype(jnp.float32)
            mean = jnp.mean(wide * wide, axis=-1, keepdims=True)
            wide = wide * lax.rsqrt(mean + 1e-06) * gains
            out = wide * cosines[rows, :] + pltpu.roll(wide, HALF, 1) * sines[rows, :]
            turned[s, rows, :] = out
            largest = jnp.maximum(
                largest, jnp.max(jnp.abs(out).reshape(CHUNK // 8, 8, LANES), axis=0)
            )
        maxes[0, pl.ds(s, 1), :] = jnp.max(largest, axis=0, keepdims=True)
        return 0

    lax.fori_loop(0, SEQS, turn_sequence, 0)

    first = plan(maxes.at[0], maxes.at[1], 0, 1, 0, max_sem.at[0], max_sem.at[1])
    first.start()
    start(vz[Z_FIRST:])
    start(along_z(0, values, vland))
    start(along_x(0, values, vland, FIRST_ROWS, ROWS - FIRST_ROWS))
    for i in range(V_ONE):
        vz[i].wait_recv()
        vf[i].start()
    first.wait()
    maxes[2] = jnp.maximum(maxes[0], maxes[1])
    second = [
        plan(maxes.at[2], maxes.at[3 + i], dx, 0, dc, max_sem.at[2], max_sem.at[3])
        for dx, dc, i in steps + [(0, 1, RELAYED)]
    ]
    start(second)
    for i in range(V_ONE, V_TWO):
        vz[i].wait_recv()
        vf[i].start()
    wait_for(maxes.at[pl.ds(3, PLANE)], max_sem.at[3])
    largest = maxes[2]
    for i in range(PLANE):
        largest = jnp.maximum(largest, maxes[3 + i])
    maxes[0] = largest
    scale[...] = maxes[0, pl.ds(me, 1), :]

    def scale_sequence(s, _):
        inverse = 1.0 / maxes[0, pl.ds(s, 1), :]
        for c in range(ROWS // CHUNK):
            rows = pl.ds(c * CHUNK, CHUNK)
            narrow[s, rows, :] = (turned[s, rows, :] * inverse).astype(jnp.bfloat16)
        return 0

    lax.fori_loop(0, SEQS, scale_sequence, 0)

    kz, kf = relay_out(1, narrow, krelay), forward(1, krelay, kland)
    start(kz + along_z(1, narrow, kland))
    for i in range(V_TWO, RELAYED):
        vz[i].wait_recv()
        vf[i].start()
    start(along_x(1, narrow, kland, 0, ROWS) + to_sibling(1, narrow, kland))

    def keep_rows(c, _):
        kland[block(me, c * CHUNK, CHUNK), :] = narrow[
            me, pl.ds(pl.multiple_of(c * CHUNK, CHUNK), CHUNK), :
        ]
        return 0

    lax.fori_loop(0, ROWS // CHUNK, keep_rows, 0)
    for i in range(RELAYED):
        kz[i].wait_recv()
        kf[i].start()
    keep.wait()
    wait_for(maxes.at[pl.ds(3, PLANE)], max_sem.at[2])
    wait_for(turned.at[pl.ds(0, RELAYED)], send_sem.at[0])
    wait_for(turned.at[pl.ds(0, 15)], send_sem.at[1])
    wait_for(turned.at[pl.ds(0, 15)], land_sem.at[0])


PIECES = 2


def store(kland, vland, scale, kout, vout, scale_out, sems):
    rows = TOTAL // PIECES
    copies = []
    for i, (source, target) in enumerate(((kland, kout), (vland, vout))):
        for j in range(PIECES):
            part = pl.ds(j * rows, rows)
            copies.append(pltpu.make_async_copy(source.at[part], target.at[part], sems.at[i, j]))
    copies.append(pltpu.make_async_copy(scale, scale_out, sems.at[2, 0]))
    for copy in copies:
        copy.start()
    for copy in copies:
        copy.wait()


def local(raw_keys, raw_values, turn_angle, key_gain):
    shape = (SEQS, ROWS, LANES)
    hbm = pl.BlockSpec(memory_space=pltpu.HBM)
    vmem = pl.BlockSpec(memory_space=pltpu.VMEM)
    kland, vland, scale = pl.pallas_call(
        exchange,
        name="exchange",
        out_shape=(
            pltpu.VMEM((TOTAL, LANES), jnp.bfloat16),
            pltpu.VMEM((TOTAL, LANES), jnp.bfloat16),
            pltpu.VMEM((1, LANES), jnp.float32),
        ),
        in_specs=[hbm, hbm, hbm, hbm],
        out_specs=(vmem, vmem, vmem),
        scratch_shapes=[
            pltpu.VMEM(shape, jnp.bfloat16),
            pltpu.VMEM(shape, jnp.float32),
            pltpu.VMEM(shape, jnp.bfloat16),
            pltpu.VMEM((RELAYED, ROWS, LANES), jnp.bfloat16),
            pltpu.VMEM((RELAYED, ROWS, LANES), jnp.bfloat16),
            pltpu.VMEM((HALF, ROWS), jnp.float32),
            pltpu.VMEM((1, LANES), jnp.float32),
            pltpu.VMEM((ROWS, LANES), jnp.float32),
            pltpu.VMEM((ROWS, LANES), jnp.float32),
            pltpu.VMEM((3 + PLANE, SEQS, LANES), jnp.float32),
            pltpu.SemaphoreType.DMA((4,)),
            pltpu.SemaphoreType.REGULAR,
            pltpu.SemaphoreType.DMA((2,)),
            pltpu.SemaphoreType.DMA((1,)),
            pltpu.SemaphoreType.DMA((2, RELAYED)),
            pltpu.SemaphoreType.DMA((4,)),
        ],
        compiler_params=pltpu.CompilerParams(
            collective_id=0, has_side_effects=True, vmem_limit_bytes=40 * 2**20
        ),
    )(
        *(
            pltpu.with_memory_space_constraint(array, pltpu.HBM)
            for array in (
                raw_keys.reshape(shape),
                raw_values.reshape(shape),
                turn_angle.T,
                key_gain.reshape(1, LANES),
            )
        )
    )
    kout, vout, scale = pl.pallas_call(
        store,
        name="store",
        out_shape=(
            jax.ShapeDtypeStruct((TOTAL, LANES), jnp.bfloat16),
            jax.ShapeDtypeStruct((TOTAL, LANES), jnp.bfloat16),
            jax.ShapeDtypeStruct((1, LANES), jnp.float32),
        ),
        in_specs=[vmem, vmem, vmem],
        out_specs=(hbm, hbm, hbm),
        scratch_shapes=[pltpu.SemaphoreType.DMA((3, PIECES))],
        compiler_params=pltpu.CompilerParams(vmem_limit_bytes=2**20),
    )(kland, vland, scale)
    whole = (1, TOTAL, 1, LANES)
    return kout.reshape(whole), vout.reshape(whole), scale.reshape(1, 1, LANES)


def solution(mesh):
    in_specs = (
        P(None, ("farcp", "nearcp"), "model", None),
        P(None, ("farcp", "nearcp"), "model", None),
        P(),
        P(),
    )
    out_specs = (
        P(("farcp", "nearcp"), None, "model", None),
        P(("farcp", "nearcp"), None, "model", None),
        P(("farcp", "nearcp"), "model", None),
    )
    return jax.shard_map(local, mesh=mesh, in_specs=in_specs, out_specs=out_specs, check_vma=False)
```

```python
import jax
import jax.numpy as jnp
from jax import lax
from jax.experimental import pallas as pl
from jax.experimental.pallas import tpu as pltpu
from jax.sharding import PartitionSpec as P

MESH = pl.DeviceIdType.MESH
SEQS, ROWS, LANES, HALF = 16, 1024, 128, 64
TOTAL = SEQS * ROWS
CHUNK = 128
FIRST_ROWS = 896
Z_FIRST = 4
V_ONE, V_TWO = 3, 6


ALONG_X = (1, 3, 2)
RELAYED = 2 * len(ALONG_X)
PLANE = RELAYED + 1
ARRIVING = 15 * ROWS


def exchange(
    keys, values, angle, gain,
    kland, vland, scale,
    raw, turned, narrow, krelay, vrelay, angles, gains_row, cosines, sines, maxes,
    local_sem, ready_sem, send_sem, land_sem, hop_sem, max_sem,
):
    far, near, model = lax.axis_index("farcp"), lax.axis_index("nearcp"), lax.axis_index("model")
    core, x, z = lax.rem(near, 2), lax.rem(lax.div(near, 2), 2) * 2 + far, lax.div(near, 4)

    def place(dx, dz, dc):
        px, pz, pc = lax.rem(x + dx, 4), lax.rem(z + dz, 2), lax.rem(core + dc, 2)
        return lax.rem(px, 2), pz * 4 + lax.div(px, 2) * 2 + pc

    def device(dx, dz, dc):
        return (*place(dx, dz, dc), model)

    def index(dx, dz, dc):
        f, n = place(dx, dz, dc)
        return f * 8 + n

    def block(owner, first=0, rows=ROWS):
        return pl.ds(pl.multiple_of(owner * ROWS + first, CHUNK), rows)

    me, across = far * 8 + near, index(0, 1, 0)

    turns = ((1, (0, 1, 2)), (0, (2, 0, 1)))
    steps = [(ALONG_X[n], lax.rem(core + to, 2), n) for to, order in turns for n in order]
    steps = [(dx, dc, n + len(ALONG_X) * dc) for dx, dc, n in steps]

    def plan(source, target, dx, dz, dc, sent, arrived):
        return pltpu.make_async_remote_copy(
            src_ref=source,
            dst_ref=target,
            send_sem=sent,
            recv_sem=arrived,
            device_id=device(dx, dz, dc),
            device_id_type=MESH,
        )

    def wait_for(ref, sem):
        pltpu.make_async_copy(ref, ref, sem).wait()

    def start(copies):
        for copy in copies:
            copy.start()

    load_keys = pltpu.make_async_copy(keys, raw, local_sem.at[0])
    load_angles = pltpu.make_async_copy(angle.at[:, block(me)], angles, local_sem.at[1])
    load_gain = pltpu.make_async_copy(gain, gains_row, local_sem.at[2])
    keep = pltpu.make_async_copy(values.at[me], vland.at[block(me)], local_sem.at[3])

    barrier = pltpu.get_barrier_semaphore()
    greeted = [device(0, 1, core), device(0, 0, 1)] + [device(dx, 0, 1 - core) for dx in (1, 3, 2)]
    for target in greeted:
        pl.semaphore_signal(barrier, inc=1, device_id=target, device_id_type=MESH)
    load_angles.start()
    load_gain.start()
    load_keys.start()
    pl.semaphore_wait(barrier, 3 + 4 * core)
    pl.semaphore_signal(ready_sem, inc=1, device_id=device(0, 0, 1), device_id_type=MESH)

    def relay_out(n, source, relay):
        return [
            plan(
                source.at[index(dx, 1, dc)], relay.at[i],
                0, 1, 0, send_sem.at[n], hop_sem.at[n, i],
            )
            for dx, dc, i in steps
        ]

    def forward(n, relay, land):
        return [
            plan(
                relay.at[i], land.at[block(across)],
                dx, 0, dc, send_sem.at[2 + n], land_sem.at[n],
            )
            for dx, dc, i in steps
        ]

    def along_x(n, source, land, first, rows):
        part = pl.ds(first, rows)
        return [
            plan(
                source.at[index(dx, 0, dc), part], land.at[block(me, first, rows)],
                dx, 0, dc, send_sem.at[2 + n], land_sem.at[n],
            )
            for dx, dc, i in steps
        ]

    def straight(n, source, land, dz, dc):
        return plan(
            source.at[index(0, dz, dc)], land.at[block(me)],
            0, dz, dc, send_sem.at[2 + n], land_sem.at[n],
        )

    def along_z(n, source, land):
        return [straight(n, source, land, 1, dc) for dc in (1 - core, core)]

    def to_sibling(n, source, land):
        return [straight(n, source, land, 0, 1)]

    vz, vf = relay_out(0, values, vrelay), forward(0, vrelay, vland)
    vx = along_x(0, values, vland, 0, FIRST_ROWS)

    @pl.when(core == 0)
    def _():
        start(vz[:Z_FIRST])

    @pl.when(core == 1)
    def _():
        start(vx)

    pl.semaphore_wait(ready_sem, 1)

    @pl.when(core == 0)
    def _():
        start(vx)

    @pl.when(core == 1)
    def _():
        start(vz[:Z_FIRST])

    start(to_sibling(0, values, vland))
    keep.start()

    load_angles.wait()
    for c in range(ROWS // CHUNK):
        a = angles[:, c * CHUNK : (c + 1) * CHUNK]
        cosine, sine = jnp.cos(a), jnp.sin(a)
        rows = pl.ds(c * CHUNK, CHUNK)
        cosines[rows, :] = jnp.concatenate([cosine, cosine], axis=0).T
        sines[rows, :] = jnp.concatenate([-sine, sine], axis=0).T

    load_gain.wait()
    load_keys.wait()
    gains = gains_row[...]

    def turn_sequence(s, _):
        largest = jnp.zeros((8, LANES), jnp.float32)
        for c in range(ROWS // CHUNK):
            rows = pl.ds(c * CHUNK, CHUNK)
            wide = raw[s, rows, :].astype(jnp.float32)
            mean = jnp.mean(wide * wide, axis=-1, keepdims=True)
            wide = wide * lax.rsqrt(mean + 1e-06) * gains
            out = wide * cosines[rows, :] + pltpu.roll(wide, HALF, 1) * sines[rows, :]
            turned[s, rows, :] = out
            largest = jnp.maximum(
                largest, jnp.max(jnp.abs(out).reshape(CHUNK // 8, 8, LANES), axis=0)
            )
        maxes[0, pl.ds(s, 1), :] = jnp.max(largest, axis=0, keepdims=True)
        return 0

    lax.fori_loop(0, SEQS, turn_sequence, 0)

    first = plan(maxes.at[0], maxes.at[1], 0, 1, 0, max_sem.at[0], max_sem.at[1])
    first.start()
    start(vz[Z_FIRST:])
    start(along_z(0, values, vland))
    start(along_x(0, values, vland, FIRST_ROWS, ROWS - FIRST_ROWS))
    for i in range(V_ONE):
        vz[i].wait_recv()
        vf[i].start()
    first.wait()
    maxes[2] = jnp.maximum(maxes[0], maxes[1])
    second = [
        plan(maxes.at[2], maxes.at[3 + i], dx, 0, dc, max_sem.at[2], max_sem.at[3])
        for dx, dc, i in steps + [(0, 1, RELAYED)]
    ]
    start(second)
    for i in range(V_ONE, V_TWO):
        vz[i].wait_recv()
        vf[i].start()
    wait_for(maxes.at[pl.ds(3, PLANE)], max_sem.at[3])
    largest = maxes[2]
    for i in range(PLANE):
        largest = jnp.maximum(largest, maxes[3 + i])
    maxes[0] = largest
    scale[...] = maxes[0, pl.ds(me, 1), :]

    def scale_sequence(s, _):
        inverse = 1.0 / maxes[0, pl.ds(s, 1), :]
        for c in range(ROWS // CHUNK):
            rows = pl.ds(c * CHUNK, CHUNK)
            narrow[s, rows, :] = (turned[s, rows, :] * inverse).astype(jnp.bfloat16)
        return 0

    lax.fori_loop(0, SEQS, scale_sequence, 0)

    kz, kf = relay_out(1, narrow, krelay), forward(1, krelay, kland)
    start(kz + along_z(1, narrow, kland))
    for i in range(V_TWO, RELAYED):
        vz[i].wait_recv()
        vf[i].start()
    start(along_x(1, narrow, kland, 0, ROWS) + to_sibling(1, narrow, kland))

    def keep_rows(c, _):
        kland[block(me, c * CHUNK, CHUNK), :] = narrow[
            me, pl.ds(pl.multiple_of(c * CHUNK, CHUNK), CHUNK), :
        ]
        return 0

    lax.fori_loop(0, ROWS // CHUNK, keep_rows, 0)
    for i in range(RELAYED):
        kz[i].wait_recv()
        kf[i].start()
    keep.wait()
    wait_for(maxes.at[pl.ds(3, PLANE)], max_sem.at[2])
    for n, (relay, land) in enumerate(((vrelay, vland), (krelay, kland))):
        arriving = land.at[pl.ds(0, ARRIVING)]
        wait_for(relay, send_sem.at[n])
        wait_for(arriving, send_sem.at[2 + n])
        wait_for(arriving, land_sem.at[n])


PIECES = 2


def store(kland, vland, scale, kout, vout, scale_out, sems):
    rows = TOTAL // PIECES
    copies = []
    for i, (source, target) in enumerate(((kland, kout), (vland, vout))):
        for j in range(PIECES):
            part = pl.ds(j * rows, rows)
            copies.append(pltpu.make_async_copy(source.at[part], target.at[part], sems.at[i, j]))
    copies.append(pltpu.make_async_copy(scale, scale_out, sems.at[2, 0]))
    for copy in copies:
        copy.start()
    for copy in copies:
        copy.wait()


def local(raw_keys, raw_values, turn_angle, key_gain):
    shape = (SEQS, ROWS, LANES)
    hbm = pl.BlockSpec(memory_space=pltpu.HBM)
    vmem = pl.BlockSpec(memory_space=pltpu.VMEM)
    kland, vland, scale = pl.pallas_call(
        exchange,
        name="exchange",
        out_shape=(
            pltpu.VMEM((TOTAL, LANES), jnp.bfloat16),
            pltpu.VMEM((TOTAL, LANES), jnp.bfloat16),
            pltpu.VMEM((1, LANES), jnp.float32),
        ),
        in_specs=[hbm, hbm, hbm, hbm],
        out_specs=(vmem, vmem, vmem),
        scratch_shapes=[
            pltpu.VMEM(shape, jnp.bfloat16),
            pltpu.VMEM(shape, jnp.float32),
            pltpu.VMEM(shape, jnp.bfloat16),
            pltpu.VMEM((RELAYED, ROWS, LANES), jnp.bfloat16),
            pltpu.VMEM((RELAYED, ROWS, LANES), jnp.bfloat16),
            pltpu.VMEM((HALF, ROWS), jnp.float32),
            pltpu.VMEM((1, LANES), jnp.float32),
            pltpu.VMEM((ROWS, LANES), jnp.float32),
            pltpu.VMEM((ROWS, LANES), jnp.float32),
            pltpu.VMEM((3 + PLANE, SEQS, LANES), jnp.float32),
            pltpu.SemaphoreType.DMA((4,)),
            pltpu.SemaphoreType.REGULAR,
            pltpu.SemaphoreType.DMA((4,)),
            pltpu.SemaphoreType.DMA((2,)),
            pltpu.SemaphoreType.DMA((2, RELAYED)),
            pltpu.SemaphoreType.DMA((4,)),
        ],
        compiler_params=pltpu.CompilerParams(
            collective_id=0, has_side_effects=True, vmem_limit_bytes=40 * 2**20
        ),
    )(
        *(
            pltpu.with_memory_space_constraint(array, pltpu.HBM)
            for array in (
                raw_keys.reshape(shape),
                raw_values.reshape(shape),
                turn_angle.T,
                key_gain.reshape(1, LANES),
            )
        )
    )
    kout, vout, scale = pl.pallas_call(
        store,
        name="store",
        out_shape=(
            jax.ShapeDtypeStruct((TOTAL, LANES), jnp.bfloat16),
            jax.ShapeDtypeStruct((TOTAL, LANES), jnp.bfloat16),
            jax.ShapeDtypeStruct((1, LANES), jnp.float32),
        ),
        in_specs=[vmem, vmem, vmem],
        out_specs=(hbm, hbm, hbm),
        scratch_shapes=[pltpu.SemaphoreType.DMA((3, PIECES))],
        compiler_params=pltpu.CompilerParams(vmem_limit_bytes=2**20),
    )(kland, vland, scale)
    whole = (1, TOTAL, 1, LANES)
    return kout.reshape(whole), vout.reshape(whole), scale.reshape(1, 1, LANES)


def solution(mesh):
    in_specs = (
        P(None, ("farcp", "nearcp"), "model", None),
        P(None, ("farcp", "nearcp"), "model", None),
        P(),
        P(),
    )
    out_specs = (
        P(("farcp", "nearcp"), None, "model", None),
        P(("farcp", "nearcp"), None, "model", None),
        P(("farcp", "nearcp"), "model", None),
    )
    return jax.shard_map(local, mesh=mesh, in_specs=in_specs, out_specs=out_specs, check_vma=False)
```
